512 devices in a mesh: tm: 8 (over z), cell: 64 (over x, y, core).
Axes of the slice: x: 4, y: 8, z: 8, core: 2. Of those that a mesh axis runs over, the one named last changes fastest.
Arguments:
- initial: float32 [16384, 128], P('cell'), may hold values from 0.2 to 6, as said below
- source: float32 [16, 16384, 128], P('tm', 'cell'), may hold values from -1.8 to 1.8
- mix_rate: float32 [128], replicated, may hold values from 0.05 to 0.4
- fine_inverse: float32 [16, 128, 128, 128], P('tm', 'cell'), may hold values from -0.1 to 0.9, as said below
- coarse_inverse: float32 [16, 128, 128, 128], P('tm', 'cell'), may hold values from -0.1 to 1, as said below
- step_counts: int32 [16384], P('cell'), may hold values from 4 to 8
Outputs:
- finals: float32 [16, 16384, 128], P('tm', 'cell')
The draws below stay inside these ranges and needn't reach their ends.
Inputs may be any that keep to these rules, and one draw needn't show every extreme that they name: `initial`: positive compositions. `fine_inverse`: each matrix is a positive diagonal plus small off-diagonal entries. `coarse_inverse`: each matrix is a positive diagonal plus small off-diagonal entries.
All inputs are finite; a program needn't handle non-finite values.
Results may differ from the reference program's by a relative error of at most 0.00011.
Values sent between devices are 32-bit elements; how exact they have to be, the bound alone decides.
A program may use at most 64 MiB of HBM per device.

```python
import math
import jax
import jax.numpy as jnp
from jax import lax

S = 128
FINE_MAX = 8
ITERS = 2
CELLS = 16384
SLICES = 16
GROUPS = 128


def draw_initial(key, part):
    first = jax.random.fold_in(key, 0)
    base = jnp.exp(jax.random.uniform(first, (CELLS, S), jnp.float32, math.log(0.2), math.log(2.0)))
    ramp = 1.0 + 2.0 * jnp.arange(CELLS, dtype=jnp.float32)[:, None] / CELLS
    return base * ramp


def inverse_family(key, lowest, highest, spread):
    first, second = jax.random.split(key)
    diagonal = jnp.exp(jax.random.uniform(first, (SLICES, GROUPS, S), jnp.float32, math.log(lowest), math.log(highest)))
    offdiag = jnp.clip(jax.random.normal(second, (SLICES, GROUPS, S, S), jnp.float32) * spread / math.sqrt(S), -0.1, 0.1)
    return offdiag + diagonal[..., None] * jnp.eye(S, dtype=jnp.float32)


def draw_fine_inverse(key, part):
    return inverse_family(jax.random.fold_in(key, 11), 0.3, 0.8, 0.1)


def draw_coarse_inverse(key, part):
    return inverse_family(jax.random.fold_in(key, 23), 0.3, 0.9, 0.08)


def set_ends(drawn, key, smallest, largest):
    place = [jax.random.randint(jax.random.fold_in(key, axis), (), 0, length) for axis, length in enumerate(drawn.shape)]
    main_axis = drawn.shape.index(max(drawn.shape))
    beside = place[:main_axis] + [(place[main_axis] + 1) % drawn.shape[main_axis]] + place[main_axis + 1:]
    return drawn.at[tuple(place)].set(smallest).at[tuple(beside)].set(largest)


def level_of(key, extent, cuts, low, top_value):
    def one(axis_at, shards_of):
        heights = jax.random.uniform(jax.random.fold_in(jax.random.fold_in(key, 6), axis_at), (shards_of,), jnp.float32, low / len(cuts), top_value / len(cuts))
        return jnp.repeat(jnp.exp(heights), extent[axis_at] // shards_of).reshape((-1,) + (1,) * (len(extent) - axis_at - 1))

    loudness = one(*cuts[0])
    for cut in cuts[1:]:
        loudness = loudness * one(*cut)
    return loudness


def centred(stream_key, extent, scale, reach, pieces=(), kind=jnp.bfloat16):
    values = scale * jax.random.normal(stream_key, extent, jnp.float32)
    if pieces:
        values = values * level_of(stream_key, extent, pieces, -0.22, 0.18)
    return jnp.clip(values, -reach, reach).astype(kind)


def setup_inputs(seed: int = 0) -> dict:
    seeds = jax.random.split(jax.random.key(seed), 7)
    initial = draw_initial(jax.random.fold_in(seeds[6], 71), 0)
    source = centred(seeds[1], (SLICES, CELLS, S), 0.3, 1.8, ((0, 8), (1, 64)), jnp.float32)
    mix_rate = jnp.clip(jax.random.uniform(seeds[2], (S,), jnp.float32, 0.05, 0.4), 0.05, 0.4)
    fine_inverse = draw_fine_inverse(jax.random.fold_in(seeds[6], 71), 0)
    coarse_inverse = draw_coarse_inverse(jax.random.fold_in(seeds[6], 71), 0)
    step_counts = set_ends(jax.random.randint(seeds[5], (CELLS,), FINE_MAX // 2, FINE_MAX + 1), jax.random.fold_in(seeds[5], 1), FINE_MAX // 2, FINE_MAX).astype(jnp.int32)
    return dict(initial=initial, source=source, mix_rate=mix_rate, fine_inverse=fine_inverse, coarse_inverse=coarse_inverse, step_counts=step_counts)


def group_apply(state, matrices):
    lead, count, width = state.shape
    groups = matrices.shape[1]
    shaped = state.reshape(lead, groups, count // groups, width)
    result = jnp.einsum("lgcs,lgst->lgct", shaped, matrices, precision=lax.Precision.HIGHEST)
    return result.reshape(lead, count, width)


def chain(initial, offsets, coarse_inverse):
    def advance(state, inputs):
        matrices, offset = inputs
        nxt = group_apply(state[None], matrices[None])[0] + offset
        return nxt, nxt

    _, finals = lax.scan(advance, initial, (coarse_inverse, offsets))
    return finals


def reference(initial, source, mix_rate, fine_inverse, coarse_inverse, step_counts):
    offsets0 = group_apply(source, coarse_inverse)
    finals = chain(initial, offsets0, coarse_inverse)
    for sweep_round in range(ITERS):
        starts = jnp.concatenate([initial[None], finals[:-1]], axis=0)
        state = starts
        for substep in range(FINE_MAX):
            average = jnp.sum(state, axis=1, keepdims=True) / CELLS
            moved = group_apply(state + source + mix_rate * (average - state), fine_inverse)
            active = (substep < step_counts)[None, :, None]
            state = jnp.where(active, moved, state)
        coarse_ends = group_apply(starts, coarse_inverse) + offsets0
        offsets = offsets0 + state - coarse_ends
        finals = chain(initial, offsets, coarse_inverse)
    return finals
```

```python
import jax
import jax.numpy as jnp
from jax import lax
from jax.experimental import pallas as pl
from jax.experimental.pallas import tpu as pltpu
from jax.sharding import PartitionSpec as P

FINE_MAX = 8
ITERS = 2
FEWEST = 4
CLASSES = 5
MESH = pl.DeviceIdType.MESH
F32 = jnp.float32
BF16 = jnp.bfloat16
XS, YS, CORES = 4, 8, 2
NCHUNK = 8


def split(a):
    high = a.astype(BF16)
    low = (a - high.astype(F32)).astype(BF16)
    return jnp.concatenate([high, low], axis=1)


def put_weights(ref, matrix):
    width = matrix.shape[0]
    pair = split(matrix)
    ref[0:width, :] = pair
    ref[width : 2 * width, :] = pair


def halves(a):
    width = a.shape[1] // 2
    return a[:, :width] + a[:, width:]


def mul(a, weights):
    return halves(jnp.dot(split(a), weights[...], preferred_element_type=F32))


def class_sums(onehot, cells):
    return halves(jnp.dot(onehot, split(cells), preferred_element_type=F32))


def pick(rows, counts):
    out = jnp.broadcast_to(rows[0:1], counts.shape)
    for j in range(1, CLASSES):
        out = jnp.where(counts == float(FEWEST + j), rows[j : j + 1], out)
    return out


def cell_peers():
    me = lax.axis_index("cell")
    core, y, x = me % CORES, (me // CORES) % YS, me // (CORES * YS)
    steps = [
        (min(dx, XS - dx) + min(dy, YS - dy), dx, dy, dc)
        for dx in range(XS)
        for dy in range(YS)
        for dc in range(CORES)
        if dx or dy or dc
    ]
    steps.sort(reverse=True)
    return [
        (((x + dx) % XS) * YS + (y + dy) % YS) * CORES + (core + dc) % CORES
        for _, dx, dy, dc in steps
    ]


def kernel(
    initial, source, mix, fine, coarse, steps, out,
    wf, wc, wp, state, starts, off, shifted, counts, sums, weights_n,
    sbuf, rbuf, zs, zr, ssem, rsem, zssem, zrsem,
):
    lead, count, width = source.shape
    groups = fine.shape[1]
    per = count // groups
    tm = lax.axis_index("tm")
    last = lax.axis_size("tm") - 1
    peers = cell_peers()
    cells = count * lax.axis_size("cell")
    chunk = count // NCHUNK

    barrier = pltpu.get_barrier_semaphore()
    for peer in peers:
        pl.semaphore_signal(barrier, inc=1, device_id={"cell": peer}, device_id_type=MESH)
    behind = lax.rem(tm + last, last + 1)
    pl.semaphore_signal(barrier, inc=1, device_id={"tm": behind}, device_id_type=MESH)

    def rows(g):
        return pl.ds(g * per, per)

    rate = mix[...]
    keep = 1.0 - rate
    row_ids = lax.broadcasted_iota(jnp.int32, (8, width), 0)
    limits = jnp.concatenate([jnp.where(row_ids < CLASSES, row_ids + FEWEST, 0)] * 2, axis=0)
    onehots = []
    for g in range(groups):
        for l in range(lead):
            put_weights(wf.at[l, g], fine[l, g])
            put_weights(wc.at[l, g], coarse[l, g])
        put_weights(wp.at[g], mul(coarse[0, g], wc.at[1, g]))
        line = steps[g : g + 1, :]
        hot = jnp.where(line == row_ids + FEWEST, 1.0, 0.0).astype(F32)
        onehots.append(hot.astype(BF16))
        number = jnp.sum(hot, axis=1, keepdims=True)
        ones = jnp.where(row_ids < CLASSES, 1.0, 0.0).astype(F32)
        weights_n[g] = jnp.concatenate([number * rate, ones * rate], axis=0)
        counts[g] = jnp.broadcast_to(line.astype(F32), (per, width)).T
        for l in range(lead):
            cells_l = source[l, rows(g)]
            summed = class_sums(onehots[g], cells_l)
            sums[l, g] = jnp.concatenate([summed, jnp.zeros_like(summed)], axis=0)
            off[l, rows(g)] = mul(cells_l, wc.at[l, g])
        shifted[rows(g)] = mul(off[0, rows(g)], wc.at[1, g]) + off[1, rows(g)]

    @pl.when(tm == 0)
    def _():
        for k in range(ITERS + 1):
            zr[k] = initial[...]

    pl.semaphore_wait(barrier, len(peers) + 1)

    def hop(k, j):
        part = pl.ds(j * chunk, chunk)
        return pltpu.make_async_remote_copy(
            src_ref=zs.at[k, part],
            dst_ref=zr.at[k, part],
            send_sem=zssem.at[k * NCHUNK + j],
            recv_sem=zrsem.at[k * NCHUNK + j],
            device_id={"tm": lax.rem(tm + 1, last + 1)},
            device_id_type=MESH,
        )

    def chain(k):
        for j in range(NCHUNK):
            part = pl.ds(j * chunk, chunk)

            @pl.when(tm > 0)
            def _():
                hop(k, j).wait_recv()

            ending = mul(zr[k, part], wp.at[j * chunk // per]) + shifted[part]
            zs[k, part] = ending

            @pl.when(tm < last)
            def _():
                hop(k, j).start()

    chain(0)

    def sweep(it, carry):
        y = {}
        for g in range(groups):
            first = zr[it, rows(g)]
            second = mul(first, wc.at[0, g]) + off[0, rows(g)]
            starts[1, rows(g)] = second
            for l, begin in ((0, first), (1, second)):
                state[l, rows(g)] = begin
                summed = class_sums(onehots[g], begin)
                y[l, g] = jnp.concatenate([summed, jnp.zeros_like(summed)], axis=0)

        def fine_cells(m):
            for l in range(lead):
                for g in range(groups):
                    old = state[l, rows(g)]
                    new = mul(old * keep + source[l, rows(g)], wf.at[l, g])
                    if m >= FEWEST:
                        new = jnp.where(counts[g] > float(m), new, old)
                    state[l, rows(g)] = new

        for m in range(FINE_MAX):
            turn = it * FINE_MAX + m
            own = jnp.concatenate(
                [
                    jnp.sum(sum(y[l, g][0:8] for g in range(groups)), axis=0, keepdims=True)
                    for l in range(lead)
                ],
                axis=0,
            )
            sbuf[turn] = own
            for slot, peer in enumerate(peers):
                pltpu.make_async_remote_copy(
                    src_ref=sbuf.at[turn],
                    dst_ref=rbuf.at[turn, slot],
                    send_sem=ssem.at[turn],
                    recv_sem=rsem.at[turn],
                    device_id={"cell": peer},
                    device_id_type=MESH,
                ).start()
            if m < FINE_MAX // 2:
                fine_cells(2 * m)
                fine_cells(2 * m + 1)
            elif m == FINE_MAX // 2:
                for g in range(groups):
                    for l in range(lead):
                        begin = zr[it, rows(g)] if l == 0 else starts[1, rows(g)]
                        off[l, rows(g)] = state[l, rows(g)] - mul(begin, wc.at[l, g])
                    shifted[rows(g)] = mul(off[0, rows(g)], wc.at[1, g]) + off[1, rows(g)]
            pltpu.make_async_copy(rbuf.at[turn], rbuf.at[turn], rsem.at[turn]).wait()
            average = (own + jnp.sum(rbuf[turn], axis=0)) * (1.0 / cells)
            for l in range(lead):
                for g in range(groups):
                    old = y[l, g]
                    fed = old * keep + weights_n[g] * average[l : l + 1] + sums[l, g]
                    new = mul(fed, wf.at[l, g])
                    y[l, g] = jnp.where(limits > m, new, old) if m >= FEWEST else new
        for g in range(groups):
            extra = mul(y[0, g], wc.at[1, g]) + y[1, g]
            shifted[rows(g)] += pick(extra[8:16], counts[g])
        chain(it + 1)
        for g in range(groups):
            off[0, rows(g)] += pick(y[0, g][8:16], counts[g])
        return carry

    lax.fori_loop(0, ITERS, sweep, 0)

    for g in range(groups):
        out[0, rows(g)] = mul(zr[ITERS, rows(g)], wc.at[0, g]) + off[0, rows(g)]
        out[1, rows(g)] = zs[ITERS, rows(g)]

    def drain(turn, carry):
        pltpu.make_async_copy(rbuf.at[turn], rbuf.at[turn], ssem.at[turn]).wait()
        return carry

    lax.fori_loop(0, ITERS * FINE_MAX, drain, 0)

    @pl.when(tm < last)
    def _():
        for k in range(ITERS + 1):
            for j in range(NCHUNK):
                hop(k, j).wait_send()


def body(initial, source, mix_rate, fine_inverse, coarse_inverse, step_counts):
    lead, count, width = source.shape
    groups = fine_inverse.shape[1]
    turns = ITERS * FINE_MAX
    peers = XS * YS * CORES - 1
    vmem = pl.BlockSpec(memory_space=pltpu.VMEM)
    return pl.pallas_call(
        kernel,
        out_shape=jax.ShapeDtypeStruct(source.shape, F32),
        in_specs=[vmem] * 6,
        out_specs=vmem,
        scratch_shapes=[
            pltpu.VMEM((lead, groups, 2 * width, 2 * width), BF16),
            pltpu.VMEM((lead, groups, 2 * width, 2 * width), BF16),
            pltpu.VMEM((groups, 2 * width, 2 * width), BF16),
            pltpu.VMEM((lead, count, width), F32),
            pltpu.VMEM((lead, count, width), F32),
            pltpu.VMEM((lead, count, width), F32),
            pltpu.VMEM((count, width), F32),
            pltpu.VMEM((groups, count // groups, width), F32),
            pltpu.VMEM((lead, groups, 16, width), F32),
            pltpu.VMEM((groups, 16, width), F32),
            pltpu.VMEM((turns, lead, width), F32),
            pltpu.VMEM((turns, peers, lead, width), F32),
            pltpu.VMEM((ITERS + 1, count, width), F32),
            pltpu.VMEM((ITERS + 1, count, width), F32),
            pltpu.SemaphoreType.DMA((turns,)),
            pltpu.SemaphoreType.DMA((turns,)),
            pltpu.SemaphoreType.DMA(((ITERS + 1) * NCHUNK,)),
            pltpu.SemaphoreType.DMA(((ITERS + 1) * NCHUNK,)),
        ],
        compiler_params=pltpu.CompilerParams(collective_id=0, has_side_effects=True),
    )(
        initial,
        source,
        mix_rate.reshape(1, width),
        fine_inverse,
        coarse_inverse,
        step_counts.reshape(groups, count // groups),
    )


def solution(mesh):
    return jax.shard_map(
        body,
        mesh=mesh,
        in_specs=(
            P("cell", None),
            P("tm", "cell", None),
            P(),
            P("tm", "cell", None, None),
            P("tm", "cell", None, None),
            P("cell"),
        ),
        out_specs=P("tm", "cell", None),
        check_vma=False,
    )
```

```python
import jax
import jax.numpy as jnp
from jax import lax
from jax.experimental import pallas as pl
from jax.experimental.pallas import tpu as pltpu
from jax.sharding import PartitionSpec as P

FINE_MAX = 8
ITERS = 2
FEWEST = 4
CLASSES = 5
MESH = pl.DeviceIdType.MESH
F32 = jnp.float32
BF16 = jnp.bfloat16
XS, YS, CORES = 4, 8, 2
NCHUNK = 8


def split(a):
    high = a.astype(BF16)
    low = (a - high.astype(F32)).astype(BF16)
    return jnp.concatenate([high, low], axis=1)


def put_weights(ref, matrix):
    width = matrix.shape[0]
    pair = split(matrix)
    ref[0:width, :] = pair
    ref[width : 2 * width, :] = pair


def halves(a):
    width = a.shape[1] // 2
    return a[:, :width] + a[:, width:]


def mul(a, weights):
    return halves(jnp.dot(split(a), weights[...], preferred_element_type=F32))


def class_sums(onehot, cells):
    return halves(jnp.dot(onehot, split(cells), preferred_element_type=F32))


def pick(rows, counts):
    out = jnp.broadcast_to(rows[0:1], counts.shape)
    for j in range(1, CLASSES):
        out = jnp.where(counts == float(FEWEST + j), rows[j : j + 1], out)
    return out


def cell_place():
    me = lax.axis_index("cell")
    return me // (CORES * YS), (me // CORES) % YS, me % CORES


def cell_index(x, y, core):
    return (x * YS + y) * CORES + core


def farthest_first(xs, ys, cores):
    x, y, core = cell_place()
    moves = [
        (min(dx, XS - dx) + min(dy, YS - dy), dx, dy, dc)
        for dx in range(xs)
        for dy in range(ys)
        for dc in range(cores)
        if dx or dy or dc
    ]
    moves.sort(reverse=True)
    return [
        cell_index((x + dx) % XS, (y + dy) % YS, (core + dc) % CORES) for _, dx, dy, dc in moves
    ]


def total_rows(a):
    return jnp.sum(a, axis=0, keepdims=True)


def arrived(ref, sem):
    pltpu.make_async_copy(ref, ref, sem).wait()


def kernel(
    initial, source, mix, fine, coarse, steps, out,
    wf, wc, wp, wk, state, starts, off, shifted, counts, sums, weights_n,
    sbuf, rbuf, pair_s, pair_r, many_s, many_r, zs, zr,
    kl, kd, ks, kx, kr, ky, kf, kg, kall,
    ssem, rsem, pssem, prsem, mssem, mrsem, zssem, zrsem, kssem, krsem,
):
    lead, count, width = source.shape
    groups = fine.shape[1]
    per = count // groups
    tm = lax.axis_index("tm")
    last = lax.axis_size("tm") - 1
    x, y_at, core = cell_place()
    partner = cell_index(x, y_at, 1 - core)
    peers = farthest_first(XS, YS, CORES)
    far_peers = farthest_first(XS, YS, 1)
    cells = count * lax.axis_size("cell")
    chunk = count // NCHUNK
    slab = width // YS

    barrier = pltpu.get_barrier_semaphore()
    for peer in peers:
        pl.semaphore_signal(barrier, inc=1, device_id={"cell": peer}, device_id_type=MESH)
    behind = lax.rem(tm + last, last + 1)
    pl.semaphore_signal(barrier, inc=1, device_id={"tm": behind}, device_id_type=MESH)

    def rows(g):
        return pl.ds(g * per, per)

    def send(src, dst, ssem_one, rsem_one, peer):
        pltpu.make_async_remote_copy(
            src_ref=src,
            dst_ref=dst,
            send_sem=ssem_one,
            recv_sem=rsem_one,
            device_id={"cell": peer},
            device_id_type=MESH,
        ).start()

    rate = mix[...]
    keep = 1.0 - rate
    rate_down = jnp.broadcast_to(rate, (width, width)).T
    row_ids = lax.broadcasted_iota(jnp.int32, (8, width), 0)
    limits = jnp.concatenate([jnp.where(row_ids < CLASSES, row_ids + FEWEST, 0)] * 2, axis=0)
    onehots = []
    numbers = []
    for g in range(groups):
        for l in range(lead):
            put_weights(wf.at[l, g], fine[l, g])
            put_weights(wc.at[l, g], coarse[l, g])
        line = steps[g : g + 1, :]
        hot = jnp.where(line == row_ids + FEWEST, 1.0, 0.0).astype(F32)
        onehots.append(hot.astype(BF16))
        number = jnp.broadcast_to(jnp.sum(hot, axis=1, keepdims=True), (8, width))
        numbers.append(number)
        ones = jnp.where(row_ids < CLASSES, 1.0, 0.0).astype(F32)
        weights_n[g] = jnp.concatenate([number * rate, ones * rate], axis=0)
        counts[g] = jnp.broadcast_to(line.astype(F32), (per, width)).T
    for l in range(lead):
        for g in range(groups):
            over = 1.0 / cells
            six, seven = numbers[g][2:3] * over, (numbers[g][3:4] + numbers[g][4:5]) * over
            effect = rate_down * fine[l, g]
            terms = [(six + seven) * effect, seven * effect, six * effect, None]
            for d in range(4):
                terms.append(effect * (per * over))
                if d < 3:
                    effect = mul(effect * keep, wf.at[l, g])
                if d == 0:
                    terms[2] += seven * effect
            for i, term in enumerate(terms):
                if term is None:
                    kl[l, i] = jnp.zeros((width, width), F32)
                elif g == 0:
                    kl[l, i] = term
                else:
                    kl[l, i] += term
    for g in range(groups):
        put_weights(wp.at[g], mul(coarse[0, g], wc.at[1, g]))
        for l in range(lead):
            cells_l = source[l, rows(g)]
            summed = class_sums(onehots[g], cells_l)
            sums[l, g] = jnp.concatenate([summed, jnp.zeros_like(summed)], axis=0)
            off[l, rows(g)] = mul(cells_l, wc.at[l, g])
        shifted[rows(g)] = mul(off[0, rows(g)], wc.at[1, g]) + off[1, rows(g)]

    @pl.when(tm == 0)
    def _():
        for k in range(ITERS + 1):
            zr[k] = initial[...]

    pl.semaphore_wait(barrier, len(peers) + 1)

    def k_sems(stage, b):
        return kssem.at[stage * 2 + b], krsem.at[stage * 2 + b]

    def batch(b):
        return pl.ds(b * XS, XS)

    def pair_reduce_start(b):
        send(kl.at[1 - core, batch(b)], kd.at[batch(b)], *k_sems(0, b), partner)

    def x_reduce_start(b):
        arrived(kd.at[batch(b)], k_sems(0, b)[1])
        for i in range(XS):
            ks[b * XS + i] = kl[core, b * XS + i] + kd[b * XS + i]
        for slot, dx in enumerate((2, 1, 3)):
            to = (x + dx) % XS
            send(ks.at[b * XS + to], kx.at[b, slot], *k_sems(1, b), cell_index(to, y_at, core))

    def y_reduce_start(b):
        arrived(kx.at[b], k_sems(1, b)[1])
        kr[b] = ks[b * XS + x] + kx[b, 0] + kx[b, 1] + kx[b, 2]
        for slot, dy in enumerate((4, 3, 5, 2, 6, 1, 7)):
            to = (y_at + dy) % YS
            part = pl.ds(pl.multiple_of(to * slab, slab), slab)
            send(kr.at[b, part], ky.at[b, slot], *k_sems(2, b), cell_index(x, to, core))

    def y_gather_start(b):
        arrived(ky.at[b], k_sems(2, b)[1])
        part = pl.ds(pl.multiple_of(y_at * slab, slab), slab)
        piece = kr[b, part] + jnp.sum(ky[b], axis=0)
        kf[b] = piece
        kg[b, part] = piece
        for dy in (4, 3, 5, 2, 6, 1, 7):
            send(kf.at[b], kg.at[b, part], *k_sems(3, b), cell_index(x, (y_at + dy) % YS, core))

    def x_gather_start(b):
        arrived(ky.at[b], k_sems(3, b)[1])
        kall[core, b * XS + x] = kg[b]
        for dx in (2, 1, 3):
            send(
                kg.at[b], kall.at[core, b * XS + x], *k_sems(4, b),
                cell_index((x + dx) % XS, y_at, core),
            )

    def pair_gather_start(b):
        arrived(kx.at[b], k_sems(4, b)[1])
        send(kall.at[core, batch(b)], kall.at[core, batch(b)], *k_sems(5, b), partner)

    def k_finish(b):
        arrived(kall.at[1 - core, batch(b)], k_sems(5, b)[1])
        for l in range(lead):
            for i in range(XS):
                if b or i < 3:
                    put_weights(wk.at[l, b * XS + i], kall[l, b * XS + i])

    for b in range(2):
        pair_reduce_start(b)

    def hop(k, j):
        part = pl.ds(j * chunk, chunk)
        return pltpu.make_async_remote_copy(
            src_ref=zs.at[k, part],
            dst_ref=zr.at[k, part],
            send_sem=zssem.at[k * NCHUNK + j],
            recv_sem=zrsem.at[k * NCHUNK + j],
            device_id={"tm": lax.rem(tm + 1, last + 1)},
            device_id_type=MESH,
        )

    def chain(k):
        for j in range(NCHUNK):
            part = pl.ds(j * chunk, chunk)

            @pl.when(tm > 0)
            def _():
                hop(k, j).wait_recv()

            ending = mul(zr[k, part], wp.at[j * chunk // per]) + shifted[part]
            zs[k, part] = ending

            @pl.when(tm < last)
            def _():
                hop(k, j).start()

    def exchange_one(turn, own, work):
        sbuf[turn] = own
        for slot, peer in enumerate(peers):
            send(sbuf.at[turn], rbuf.at[turn, slot], ssem.at[turn], rsem.at[turn], peer)
        work()
        arrived(rbuf.at[turn], rsem.at[turn])
        return (own + jnp.sum(rbuf[turn], axis=0)) * (1.0 / cells)

    def exchange_many(turn, own, work):
        size = own.shape[0]
        part = pl.ds(0, size)
        pair_s[turn, part] = own
        send(pair_s.at[turn, part], pair_r.at[turn, part], pssem.at[turn], prsem.at[turn], partner)
        arrived(pair_r.at[turn, part], prsem.at[turn])
        both = own + pair_r[turn, part]
        many_s[turn, part] = both
        for slot, peer in enumerate(far_peers):
            send(
                many_s.at[turn, part], many_r.at[turn, slot, part],
                mssem.at[turn], mrsem.at[turn], peer,
            )
        work()
        whole = many_r.at[turn, pl.ds(0, len(far_peers)), part]
        arrived(whole, mrsem.at[turn])
        return (both + jnp.sum(many_r[turn, :, part], axis=0)) * (1.0 / cells)

    def partial(y, l):
        return total_rows(sum(y[l, g][0:8] for g in range(groups)))

    def advance(y, m, average):
        made = {}
        for l in range(lead):
            for g in range(groups):
                old = y[l, g]
                fed = old * keep + sums[l, g, 0 : old.shape[0]]
                if average is not None:
                    fed = fed + weights_n[g] * average[l]
                new = mul(fed, wf.at[l, g])
                made[l, g] = jnp.where(limits[0 : old.shape[0]] > m, new, old) if m >= FEWEST else new
        return made

    def fine_cells(m):
        for l in range(lead):
            for g in range(groups):
                old = state[l, rows(g)]
                new = mul(old * keep + source[l, rows(g)], wf.at[l, g])
                if m >= FEWEST:
                    new = jnp.where(counts[g] > float(m), new, old)
                state[l, rows(g)] = new

    def offsets(it):
        for g in range(groups):
            for l in range(lead):
                begin = zr[it, rows(g)] if l == 0 else starts[1, rows(g)]
                off[l, rows(g)] = state[l, rows(g)] - mul(begin, wc.at[l, g])
            shifted[rows(g)] = mul(off[0, rows(g)], wc.at[1, g]) + off[1, rows(g)]

    def through(row, l, i):
        return mul(jnp.broadcast_to(row, (8, width)), wk.at[l, i])[0:1]

    def begin(it):
        y = {}
        for g in range(groups):
            first = zr[it, rows(g)]
            second = mul(first, wc.at[0, g]) + off[0, rows(g)]
            starts[1, rows(g)] = second
            for l, cells_l in ((0, first), (1, second)):
                state[l, rows(g)] = cells_l
                summed = class_sums(onehots[g], cells_l)
                y[l, g] = jnp.concatenate([summed, jnp.zeros_like(summed)], axis=0)
        return y

    def late(y, turn, work):
        free = [y]
        for m in (5, 6):
            tops = {k: v[0:8] for k, v in free[-1].items()}
            free.append(advance(tops, m, None))
        own = jnp.concatenate([partial(f, l) for l in range(lead) for f in free], axis=0)
        got = exchange_many(turn, own, work)
        fifth = [got[3 * l : 3 * l + 1] for l in range(lead)]
        y = advance(y, 5, fifth)
        sixth = [got[3 * l + 1 : 3 * l + 2] + through(fifth[l], l, 0) for l in range(lead)]
        seventh = [got[3 * l + 2 : 3 * l + 3] + through(fifth[l], l, 2) for l in range(lead)]
        y = advance(y, 6, sixth)
        seventh = [seventh[l] + through(sixth[l], l, 1) for l in range(lead)]
        return advance(y, 7, seventh)

    def finish(y, it):
        for g in range(groups):
            extra = mul(y[0, g], wc.at[1, g]) + y[1, g]
            shifted[rows(g)] += pick(extra[8:16], counts[g])
        chain(it + 1)
        for g in range(groups):
            off[0, rows(g)] += pick(y[0, g][8:16], counts[g])

    chain(0)
    y = begin(0)

    def beside(m):
        def work():
            if m < 4:
                fine_cells(2 * m)
                fine_cells(2 * m + 1)
            if m == 0:
                x_reduce_start(0)
            elif m == 1:
                y_reduce_start(0)
                x_reduce_start(1)
            elif m == 2:
                y_gather_start(0)
            elif m == 3:
                x_gather_start(0)
                y_reduce_start(1)
            elif m == 4:
                offsets(0)
                pair_gather_start(0)
                y_gather_start(1)
            else:
                k_finish(0)
                x_gather_start(1)

        return work

    for m in range(5):
        own = jnp.concatenate([partial(y, l) for l in range(lead)], axis=0)
        average = exchange_one(m, own, beside(m))
        y = advance(y, m, [average[l : l + 1] for l in range(lead)])
    y = late(y, 0, beside(5))
    finish(y, 0)

    y = begin(1)
    free = [{k: v[0:8] for k, v in y.items()}]
    for m in range(4):
        free.append(advance(free[-1], m, None))
    own = jnp.concatenate([partial(f, l) for l in range(lead) for f in free], axis=0)

    def work():
        pair_gather_start(1)
        for m in range(FINE_MAX):
            fine_cells(m)
        k_finish(1)

    got = exchange_many(1, own, work)
    averages = [[got[5 * l + m : 5 * l + m + 1] for m in range(5)] for l in range(lead)]
    for m in range(4):
        for l in range(lead):
            for later in range(m + 1, 5):
                averages[l][later] += through(averages[l][m], l, XS + later - m - 1)
    for m in range(5):
        y = advance(y, m, [averages[l][m] for l in range(lead)])
    y = late(y, 2, lambda: offsets(1))
    finish(y, 1)

    for g in range(groups):
        out[0, rows(g)] = mul(zr[ITERS, rows(g)], wc.at[0, g]) + off[0, rows(g)]
        out[1, rows(g)] = zs[ITERS, rows(g)]

    def drain(turn, carry):
        arrived(rbuf.at[turn], ssem.at[turn])
        return carry

    lax.fori_loop(0, 5, drain, 0)
    for turn, size in ((0, 6), (1, 10), (2, 6)):
        part = pl.ds(0, size)
        arrived(pair_s.at[turn, part], pssem.at[turn])
        arrived(many_r.at[turn, pl.ds(0, len(far_peers)), part], mssem.at[turn])
    for b in range(2):
        for stage, ref in enumerate((kd.at[batch(b)], kx.at[b], ky.at[b], ky.at[b], kx.at[b], kd.at[batch(b)])):
            arrived(ref, k_sems(stage, b)[0])

    @pl.when(tm < last)
    def _():
        for k in range(ITERS + 1):
            for j in range(NCHUNK):
                hop(k, j).wait_send()


def body(initial, source, mix_rate, fine_inverse, coarse_inverse, step_counts):
    lead, count, width = source.shape
    groups = fine_inverse.shape[1]
    peers = XS * YS * CORES - 1
    far = XS * YS - 1
    mats = 2 * XS
    vmem = pl.BlockSpec(memory_space=pltpu.VMEM)
    return pl.pallas_call(
        kernel,
        out_shape=jax.ShapeDtypeStruct(source.shape, F32),
        in_specs=[vmem] * 6,
        out_specs=vmem,
        scratch_shapes=[
            pltpu.VMEM((lead, groups, 2 * width, 2 * width), BF16),
            pltpu.VMEM((lead, groups, 2 * width, 2 * width), BF16),
            pltpu.VMEM((groups, 2 * width, 2 * width), BF16),
            pltpu.VMEM((lead, mats, 2 * width, 2 * width), BF16),
            pltpu.VMEM((lead, count, width), F32),
            pltpu.VMEM((lead, count, width), F32),
            pltpu.VMEM((lead, count, width), F32),
            pltpu.VMEM((count, width), F32),
            pltpu.VMEM((groups, count // groups, width), F32),
            pltpu.VMEM((lead, groups, 16, width), F32),
            pltpu.VMEM((groups, 16, width), F32),
            pltpu.VMEM((5, lead, width), F32),
            pltpu.VMEM((5, peers, lead, width), F32),
            pltpu.VMEM((3, 16, width), F32),
            pltpu.VMEM((3, 16, width), F32),
            pltpu.VMEM((3, 16, width), F32),
            pltpu.VMEM((3, far, 16, width), F32),
            pltpu.VMEM((ITERS + 1, count, width), F32),
            pltpu.VMEM((ITERS + 1, count, width), F32),
            pltpu.VMEM((lead, mats, width, width), F32),
            pltpu.VMEM((mats, width, width), F32),
            pltpu.VMEM((mats, width, width), F32),
            pltpu.VMEM((2, XS - 1, width, width), F32),
            pltpu.VMEM((2, width, width), F32),
            pltpu.VMEM((2, YS - 1, width // YS, width), F32),
            pltpu.VMEM((2, width // YS, width), F32),
            pltpu.VMEM((2, width, width), F32),
            pltpu.VMEM((lead, mats, width, width), F32),
            pltpu.SemaphoreType.DMA((5,)),
            pltpu.SemaphoreType.DMA((5,)),
            pltpu.SemaphoreType.DMA((3,)),
            pltpu.SemaphoreType.DMA((3,)),
            pltpu.SemaphoreType.DMA((3,)),
            pltpu.SemaphoreType.DMA((3,)),
            pltpu.SemaphoreType.DMA(((ITERS + 1) * NCHUNK,)),
            pltpu.SemaphoreType.DMA(((ITERS + 1) * NCHUNK,)),
            pltpu.SemaphoreType.DMA((12,)),
            pltpu.SemaphoreType.DMA((12,)),
        ],
        compiler_params=pltpu.CompilerParams(collective_id=0, has_side_effects=True),
    )(
        initial,
        source,
        mix_rate.reshape(1, width),
        fine_inverse,
        coarse_inverse,
        step_counts.reshape(groups, count // groups),
    )


def solution(mesh):
    return jax.shard_map(
        body,
        mesh=mesh,
        in_specs=(
            P("cell", None),
            P("tm", "cell", None),
            P(),
            P("tm", "cell", None, None),
            P("tm", "cell", None, None),
            P("cell"),
        ),
        out_specs=P("tm", "cell", None),
        check_vma=False,
    )
```

```python
import jax
import jax.numpy as jnp
from jax import lax
from jax.experimental import pallas as pl
from jax.experimental.pallas import tpu as pltpu
from jax.sharding import PartitionSpec as P

FINE_MAX = 8
ITERS = 2
FEWEST = 4
CLASSES = 5
MESH = pl.DeviceIdType.MESH
F32 = jnp.float32
BF16 = jnp.bfloat16
XS, YS, CORES = 4, 8, 2
NCHUNK = 8


def split(a):
    high = a.astype(BF16)
    low = (a - high.astype(F32)).astype(BF16)
    return jnp.concatenate([high, low], axis=1)


def put_weights(ref, matrix):
    width = matrix.shape[0]
    pair = split(matrix)
    ref[0:width, :] = pair
    ref[width : 2 * width, :] = pair


def halves(a):
    width = a.shape[1] // 2
    return a[:, :width] + a[:, width:]


def mul(a, weights):
    return halves(jnp.dot(split(a), weights[...], preferred_element_type=F32))


def class_sums(onehot, cells):
    return halves(jnp.dot(onehot, split(cells), preferred_element_type=F32))


def pick(rows, counts):
    out = jnp.broadcast_to(rows[CLASSES : CLASSES + 1], counts.shape)
    for j in range(1, CLASSES):
        out = jnp.where(counts == float(FEWEST + j), rows[CLASSES + j : CLASSES + j + 1], out)
    return out


def cell_place():
    me = lax.axis_index("cell")
    return me // (CORES * YS), (me // CORES) % YS, me % CORES


def cell_index(x, y, core):
    return (x * YS + y) * CORES + core


def farthest_first(xs, ys, cores):
    x, y, core = cell_place()
    moves = [
        (min(dx, XS - dx) + min(dy, YS - dy), dx, dy, dc)
        for dx in range(xs)
        for dy in range(ys)
        for dc in range(cores)
        if dx or dy or dc
    ]
    moves.sort(reverse=True)
    return [
        cell_index((x + dx) % XS, (y + dy) % YS, (core + dc) % CORES) for _, dx, dy, dc in moves
    ]


def total_rows(a):
    return jnp.sum(a, axis=0, keepdims=True)


def arrived(ref, sem):
    pltpu.make_async_copy(ref, ref, sem).wait()


def kernel(
    initial, source, mix, fine, coarse, steps, out,
    wf, wc, wp, wk, state, starts, off, shifted, counts, sums, weights_n, yinit,
    fine_p, coarse_p, begun, offy, sbuf, rbuf, many_s, many_r, zs, zr, ys, yr, fin, fin_p,
    kl, kd, ks, kx, kr, ky, kf, kg, kall,
    ssem, rsem, mssem, mrsem, zssem, zrsem, yssem, yrsem, kssem, krsem, pssem, prsem,
):
    lead, count, width = source.shape
    groups = fine.shape[1]
    every = 2 * groups
    per = count // groups
    tm = lax.axis_index("tm")
    last = lax.axis_size("tm") - 1
    x, y_at, core = cell_place()
    partner = cell_index(x, y_at, 1 - core)
    far_peers = farthest_first(XS, YS, 1)
    x_moves, y_moves = (2, 1, 3), (4, 3, 5, 2, 6, 1, 7)
    cells = count * lax.axis_size("cell")
    chunk = count // NCHUNK
    slab = width // YS
    used = 2 * CLASSES
    lead_core = core == 1

    barrier = pltpu.get_barrier_semaphore()

    def greet(peer):
        pl.semaphore_signal(barrier, inc=1, device_id={"cell": peer}, device_id_type=MESH)

    @pl.when(lead_core)
    def _():
        for peer in far_peers:
            greet(peer)

    @pl.when(jnp.logical_not(lead_core))
    def _():
        for d in x_moves:
            greet(cell_index((x + d) % XS, y_at, core))
        for d in y_moves:
            greet(cell_index(x, (y_at + d) % YS, core))

    greet(partner)
    behind = lax.rem(tm + last, last + 1)
    pl.semaphore_signal(barrier, inc=1, device_id={"tm": behind}, device_id_type=MESH)

    def rows(g):
        return pl.ds(g * per, per)

    def send(src, dst, ssem_one, rsem_one, peer):
        pltpu.make_async_remote_copy(
            src_ref=src,
            dst_ref=dst,
            send_sem=ssem_one,
            recv_sem=rsem_one,
            device_id={"cell": peer},
            device_id_type=MESH,
        ).start()

    rate = mix[...]
    keep = 1.0 - rate
    rate_down = jnp.broadcast_to(rate, (width, width)).T
    row_ids = lax.broadcasted_iota(jnp.int32, (16, width), 0)
    cell_row = row_ids[0:8] < CLASSES
    limits = jnp.where(
        row_ids < CLASSES, row_ids + FEWEST, jnp.where(row_ids < used, row_ids + FEWEST - CLASSES, 0)
    )
    shared = jnp.where(jnp.logical_and(row_ids >= CLASSES, row_ids < used), 1.0, 0.0).astype(F32)

    def padded(a):
        return jnp.concatenate([a, jnp.zeros_like(a)], axis=0)

    numbers = []
    for g in range(groups):
        for l in range(lead):
            put_weights(wf.at[l, g], fine[l, g])
            put_weights(wc.at[l, g], coarse[l, g])
        line = steps[g : g + 1, :]
        hot = jnp.where(
            jnp.logical_and(line == row_ids[0:8] + FEWEST, cell_row), 1.0, 0.0
        ).astype(F32)
        onehot = hot.astype(BF16)
        number = jnp.broadcast_to(jnp.sum(hot, axis=1, keepdims=True), (8, width))
        numbers.append(number)
        weights_n[g] = (padded(number) + shared) * rate
        counts[g] = jnp.broadcast_to(line.astype(F32), (per, width)).T
        yinit[g] = padded(class_sums(onehot, initial[rows(g)]))
        for l in range(lead):
            sums[l, g] = padded(class_sums(onehot, source[l, rows(g)]))

    def bulk_setup():
        for g in range(groups):
            put_weights(wp.at[g], mul(coarse[0, g], wc.at[1, g]))
            for l in range(lead):
                off[l, rows(g)] = mul(source[l, rows(g)], wc.at[l, g])
            shifted[rows(g)] = mul(off[0, rows(g)], wc.at[1, g]) + off[1, rows(g)]

    def condense():
        over = 1.0 / cells
        for l in range(lead):
            for g in range(groups):
                six, seven = numbers[g][2:3] * over, (numbers[g][3:4] + numbers[g][4:5]) * over
                effect = rate_down * fine[l, g]
                terms = [(six + seven) * effect, seven * effect, six * effect, None]
                for d in range(4):
                    terms.append(effect * (per * over))
                    if d < 3:
                        effect = mul(effect * keep, wf.at[l, g])
                    if d == 0:
                        terms[2] += seven * effect
                for i, term in enumerate(terms):
                    if term is None:
                        kl[l, i] = jnp.zeros((width, width), F32)
                    elif g == 0:
                        kl[l, i] = term
                    else:
                        kl[l, i] += term

    @pl.when(tm == 0)
    def _():
        for k in range(ITERS + 1):
            zr[k] = initial[...]

    def k_sems(stage, b):
        return kssem.at[stage * 2 + b], krsem.at[stage * 2 + b]

    def batch(b):
        return pl.ds(b * XS, XS)

    def pair_reduce_start(b):
        send(kl.at[1 - core, batch(b)], kd.at[batch(b)], *k_sems(0, b), partner)

    def x_reduce_start(b):
        arrived(kd.at[batch(b)], k_sems(0, b)[1])
        for i in range(XS):
            ks[b * XS + i] = kl[core, b * XS + i] + kd[b * XS + i]
        for slot, dx in enumerate(x_moves):
            to = (x + dx) % XS
            send(ks.at[b * XS + to], kx.at[b, slot], *k_sems(1, b), cell_index(to, y_at, core))

    def y_reduce_start(b):
        arrived(kx.at[b], k_sems(1, b)[1])
        kr[b] = ks[b * XS + x] + kx[b, 0] + kx[b, 1] + kx[b, 2]
        for slot, dy in enumerate(y_moves):
            to = (y_at + dy) % YS
            part = pl.ds(pl.multiple_of(to * slab, slab), slab)
            send(kr.at[b, part], ky.at[b, slot], *k_sems(2, b), cell_index(x, to, core))

    def y_gather_start(b):
        arrived(ky.at[b], k_sems(2, b)[1])
        part = pl.ds(pl.multiple_of(y_at * slab, slab), slab)
        piece = kr[b, part] + jnp.sum(ky[b], axis=0)
        kf[b] = piece
        kg[b, part] = piece
        for dy in y_moves:
            send(kf.at[b], kg.at[b, part], *k_sems(3, b), cell_index(x, (y_at + dy) % YS, core))

    def x_gather_start(b):
        arrived(ky.at[b], k_sems(3, b)[1])
        kall[core, b * XS + x] = kg[b]
        for dx in x_moves:
            send(
                kg.at[b], kall.at[core, b * XS + x], *k_sems(4, b),
                cell_index((x + dx) % XS, y_at, core),
            )

    def x_gather_done(b):
        arrived(kx.at[b], k_sems(4, b)[1])

    def pair_gather_start(b):
        x_gather_done(b)
        send(kall.at[core, batch(b)], kall.at[core, batch(b)], *k_sems(5, b), partner)

    def k_finish(b):
        arrived(kall.at[1 - core, batch(b)], k_sems(5, b)[1])
        for l in range(lead):
            for i in range(XS):
                if b or i < 3:
                    put_weights(wk.at[l, b * XS + i], kall[l, b * XS + i])

    def hop(k, j):
        part = pl.ds(j * chunk, chunk)
        return pltpu.make_async_remote_copy(
            src_ref=zs.at[k, part],
            dst_ref=zr.at[k, part],
            send_sem=zssem.at[k * NCHUNK + j],
            recv_sem=zrsem.at[k * NCHUNK + j],
            device_id={"tm": lax.rem(tm + 1, last + 1)},
            device_id_type=MESH,
        )

    def bulk_chain(k):
        for j in range(NCHUNK):
            part = pl.ds(j * chunk, chunk)

            @pl.when(tm > 0)
            def _():
                hop(k, j).wait_recv()

            zs[k, part] = mul(zr[k, part], wp.at[j * chunk // per]) + shifted[part]

            @pl.when(tm < last)
            def _():
                hop(k, j).start()

    def bulk_begin(it):
        for g in range(groups):
            first = zr[it, rows(g)]
            second = mul(first, wc.at[0, g]) + off[0, rows(g)]
            starts[1, rows(g)] = second
            state[0, rows(g)] = first
            state[1, rows(g)] = second

    def fine_cells(m):
        for l in range(lead):
            for g in range(groups):
                old = state[l, rows(g)]
                new = mul(old * keep + source[l, rows(g)], wf.at[l, g])
                if m >= FEWEST:
                    new = jnp.where(counts[g] > float(m), new, old)
                state[l, rows(g)] = new

    def bulk_offsets(it):
        for g in range(groups):
            for l in range(lead):
                begin = zr[it, rows(g)] if l == 0 else starts[1, rows(g)]
                off[l, rows(g)] = state[l, rows(g)] - mul(begin, wc.at[l, g])
            shifted[rows(g)] = mul(off[0, rows(g)], wc.at[1, g]) + off[1, rows(g)]

    def bulk_result():
        for g in range(groups):
            state[0, rows(g)] = mul(zr[ITERS, rows(g)], wc.at[0, g]) + off[0, rows(g)]

    def result(rows_of):
        for g in range(groups):
            out[0, rows(g)] = state[0, rows(g)] + pick(rows_of(0, g), counts[g])
            out[1, rows(g)] = zs[ITERS, rows(g)] + pick(rows_of(1, g), counts[g])

    def drain_common():
        for b in range(2):
            for stage, ref in enumerate((kd.at[batch(b)], kx.at[b], ky.at[b], ky.at[b], kx.at[b])):
                arrived(ref, k_sems(stage, b)[0])

        @pl.when(tm < last)
        def _():
            for k in range(ITERS + 1):
                for j in range(NCHUNK):
                    hop(k, j).wait_send()

    own_groups, partner_groups = pl.ds(0, groups), pl.ds(groups, groups)

    def shared_copies():
        pairs = [
            (fine, fine_p),
            (coarse, coarse_p),
            (weights_n.at[own_groups], weights_n.at[partner_groups]),
            (yinit.at[own_groups], yinit.at[partner_groups]),
        ]
        pairs += [(sums.at[l, own_groups], sums.at[l, partner_groups]) for l in range(lead)]
        return pairs

    @pl.when(jnp.logical_not(lead_core))
    def _():
        condense()
        pl.semaphore_wait(barrier, len(x_moves) + len(y_moves) + 2)
        for i, (src, dst) in enumerate(shared_copies()):
            send(src, dst, pssem.at[i], prsem.at[i], partner)
        pair_reduce_start(0)
        pair_reduce_start(1)
        bulk_setup()
        x_reduce_start(0)
        x_reduce_start(1)
        y_reduce_start(0)
        bulk_chain(0)
        bulk_begin(0)
        y_gather_start(0)
        for m in range(4):
            fine_cells(m)
        y_reduce_start(1)
        x_gather_start(0)
        for m in range(4, FINE_MAX):
            fine_cells(m)
        y_gather_start(1)
        pair_gather_start(0)
        bulk_offsets(0)
        x_gather_start(1)
        bulk_chain(1)
        bulk_begin(1)
        pair_gather_start(1)
        for m in range(FINE_MAX):
            fine_cells(m)
        bulk_offsets(1)
        bulk_chain(2)
        bulk_result()
        arrived(fin_p, prsem.at[7])
        result(lambda l, g: fin_p[l, g])
        for i, (src, _) in enumerate(shared_copies()):
            arrived(src, pssem.at[i])
        for b in range(2):
            arrived(kd.at[batch(b)], k_sems(5, b)[0])
        drain_common()

    @pl.when(lead_core)
    def _():
        condense()
        bulk_setup()
        pl.semaphore_wait(barrier, len(far_peers) + 2)
        pair_reduce_start(0)
        pair_reduce_start(1)
        for i, (_, dst) in enumerate(shared_copies()):
            arrived(dst, prsem.at[i])
        for g in range(groups):
            for l in range(lead):
                put_weights(wf.at[l, groups + g], fine_p[l, g])
                put_weights(wc.at[l, groups + g], coarse_p[l, g])
            put_weights(wp.at[groups + g], mul(coarse_p[0, g], wc.at[1, groups + g]))

        @pl.when(tm == 0)
        def _():
            for k in range(ITERS + 1):
                yr[k] = yinit[...]

        each = [(l, g) for l in range(lead) for g in range(every)]
        used_rows = pl.ds(0, used)

        def row_hop(k):
            return pltpu.make_async_remote_copy(
                src_ref=ys.at[k, :, used_rows],
                dst_ref=yr.at[k, :, used_rows],
                send_sem=yssem.at[k],
                recv_sem=yrsem.at[k],
                device_id={"tm": lax.rem(tm + 1, last + 1)},
                device_id_type=MESH,
            )

        def row_chain(k):
            step = [mul(offy[0, g], wc.at[1, g]) + offy[1, g] for g in range(every)]

            @pl.when(tm > 0)
            def _():
                row_hop(k).wait_recv()

            for g in range(every):
                ys[k, g] = mul(yr[k, g], wp.at[g]) + step[g]

            @pl.when(tm < last)
            def _():
                row_hop(k).start()

        def row_begin(k):
            y = {}
            for g in range(every):
                y[0, g] = yr[k, g]
                y[1, g] = mul(yr[k, g], wc.at[0, g]) + offy[0, g]
            for l, g in each:
                begun[l, g] = y[l, g]
            return y

        def row_coarse():
            for l, g in each:
                begun[l, g] = mul(begun[l, g], wc.at[l, g])

        def row_offsets(y):
            for l, g in each:
                offy[l, g] = y[l, g] - begun[l, g]

        def exchange_one(turn, own, work):
            sbuf[turn] = own
            for slot, peer in enumerate(far_peers):
                send(sbuf.at[turn], rbuf.at[turn, slot], ssem.at[turn], rsem.at[turn], peer)
            work()
            arrived(rbuf.at[turn], rsem.at[turn])
            return (own + jnp.sum(rbuf[turn], axis=0)) * (1.0 / cells)

        def exchange_many(turn, own, work):
            part = pl.ds(0, own.shape[0])
            many_s[turn, part] = own
            for slot, peer in enumerate(far_peers):
                send(
                    many_s.at[turn, part], many_r.at[turn, slot, part],
                    mssem.at[turn], mrsem.at[turn], peer,
                )
            work()
            arrived(many_r.at[turn, :, part], mrsem.at[turn])
            return (own + jnp.sum(many_r[turn, :, part], axis=0)) * (1.0 / cells)

        def partial(y, l):
            return total_rows(jnp.where(cell_row, sum(y[l, g][0:8] for g in range(every)), 0.0))

        def advance(y, m, average):
            made = {}
            for l, g in each:
                old = y[l, g]
                size = old.shape[0]
                fed = old * keep + sums[l, g, 0:size]
                if average is not None:
                    fed = fed + weights_n[g] * average[l]
                new = mul(fed, wf.at[l, g])
                made[l, g] = jnp.where(limits[0:size] > m, new, old) if m >= FEWEST else new
            return made

        def through(row, l, i):
            return mul(jnp.broadcast_to(row, (8, width)), wk.at[l, i])[0:1]

        def late(y, turn, work):
            free = [y]
            for m in (5, 6):
                tops = {k: v[0:8] for k, v in free[-1].items()}
                free.append(advance(tops, m, None))
            own = jnp.concatenate([partial(f, l) for l in range(lead) for f in free], axis=0)
            got = exchange_many(turn, own, work)
            fifth = [got[3 * l : 3 * l + 1] for l in range(lead)]
            y = advance(y, 5, fifth)
            sixth = [got[3 * l + 1 : 3 * l + 2] + through(fifth[l], l, 0) for l in range(lead)]
            seventh = [got[3 * l + 2 : 3 * l + 3] + through(fifth[l], l, 2) for l in range(lead)]
            y = advance(y, 6, sixth)
            seventh = [seventh[l] + through(sixth[l], l, 1) for l in range(lead)]
            return advance(y, 7, seventh)

        for l, g in each:
            offy[l, g] = mul(sums[l, g], wc.at[l, g])
        row_chain(0)
        y = row_begin(0)

        def beside(m):
            def work():
                if m == 0:
                    x_reduce_start(0)
                    row_coarse()
                elif m == 1:
                    y_reduce_start(0)
                    x_reduce_start(1)
                    bulk_chain(0)
                elif m == 2:
                    y_gather_start(0)
                    bulk_begin(0)
                    for i in range(4):
                        fine_cells(i)
                elif m == 3:
                    x_gather_start(0)
                    y_reduce_start(1)
                    for i in range(4, FINE_MAX):
                        fine_cells(i)
                elif m == 4:
                    y_gather_start(1)
                    x_gather_done(0)
                    bulk_offsets(0)
                else:
                    x_gather_start(1)
                    bulk_chain(1)
                    k_finish(0)

            return work

        for m in range(5):
            own = jnp.concatenate([partial(y, l) for l in range(lead)], axis=0)
            average = exchange_one(m, own, beside(m))
            y = advance(y, m, [average[l : l + 1] for l in range(lead)])
        row_offsets(late(y, 0, beside(5)))
        row_chain(1)

        y = row_begin(1)
        free = [{k: v[0:8] for k, v in y.items()}]
        for m in range(4):
            free.append(advance(free[-1], m, None))
        own = jnp.concatenate([partial(f, l) for l in range(lead) for f in free], axis=0)

        def work():
            row_coarse()
            bulk_begin(1)
            for m in range(FINE_MAX):
                fine_cells(m)
            x_gather_done(1)
            k_finish(1)

        got = exchange_many(1, own, work)
        averages = [[got[5 * l + m : 5 * l + m + 1] for m in range(5)] for l in range(lead)]
        for m in range(4):
            for l in range(lead):
                for later in range(m + 1, 5):
                    averages[l][later] += through(averages[l][m], l, XS + later - m - 1)
        for m in range(5):
            y = advance(y, m, [averages[l][m] for l in range(lead)])

        def work():
            bulk_offsets(1)
            bulk_chain(2)
            bulk_result()

        row_offsets(late(y, 2, work))
        row_chain(2)
        for g in range(every):
            fin[0, g] = mul(yr[ITERS, g], wc.at[0, g]) + offy[0, g]
            fin[1, g] = ys[ITERS, g]
        for l in range(lead):
            send(fin.at[l, partner_groups], fin_p.at[l], pssem.at[6 + l], prsem.at[7], partner)
        result(lambda l, g: fin[l, g])

        for turn in range(5):
            arrived(rbuf.at[turn], ssem.at[turn])
        for turn, size in ((0, 6), (1, 10), (2, 6)):
            arrived(many_r.at[turn, :, pl.ds(0, size)], mssem.at[turn])
        for l in range(lead):
            arrived(fin_p.at[l], pssem.at[6 + l])
        drain_common()

        @pl.when(tm < last)
        def _():
            for k in range(ITERS + 1):
                row_hop(k).wait_send()


def body(initial, source, mix_rate, fine_inverse, coarse_inverse, step_counts):
    lead, count, width = source.shape
    groups = fine_inverse.shape[1]
    every = 2 * groups
    far = XS * YS - 1
    mats = 2 * XS
    vmem = pl.BlockSpec(memory_space=pltpu.VMEM)
    return pl.pallas_call(
        kernel,
        out_shape=jax.ShapeDtypeStruct(source.shape, F32),
        in_specs=[vmem] * 6,
        out_specs=vmem,
        scratch_shapes=[
            pltpu.VMEM((lead, every, 2 * width, 2 * width), BF16),
            pltpu.VMEM((lead, every, 2 * width, 2 * width), BF16),
            pltpu.VMEM((every, 2 * width, 2 * width), BF16),
            pltpu.VMEM((lead, mats, 2 * width, 2 * width), BF16),
            pltpu.VMEM((lead, count, width), F32),
            pltpu.VMEM((lead, count, width), F32),
            pltpu.VMEM((lead, count, width), F32),
            pltpu.VMEM((count, width), F32),
            pltpu.VMEM((groups, count // groups, width), F32),
            pltpu.VMEM((lead, every, 16, width), F32),
            pltpu.VMEM((every, 16, width), F32),
            pltpu.VMEM((every, 16, width), F32),
            pltpu.VMEM((lead, groups, width, width), F32),
            pltpu.VMEM((lead, groups, width, width), F32),
            pltpu.VMEM((lead, every, 16, width), F32),
            pltpu.VMEM((lead, every, 16, width), F32),
            pltpu.VMEM((5, lead, width), F32),
            pltpu.VMEM((5, far, lead, width), F32),
            pltpu.VMEM((3, 16, width), F32),
            pltpu.VMEM((3, far, 16, width), F32),
            pltpu.VMEM((ITERS + 1, count, width), F32),
            pltpu.VMEM((ITERS + 1, count, width), F32),
            pltpu.VMEM((ITERS + 1, every, 16, width), F32),
            pltpu.VMEM((ITERS + 1, every, 16, width), F32),
            pltpu.VMEM((lead, every, 16, width), F32),
            pltpu.VMEM((lead, groups, 16, width), F32),
            pltpu.VMEM((lead, mats, width, width), F32),
            pltpu.VMEM((mats, width, width), F32),
            pltpu.VMEM((mats, width, width), F32),
            pltpu.VMEM((2, XS - 1, width, width), F32),
            pltpu.VMEM((2, width, width), F32),
            pltpu.VMEM((2, YS - 1, width // YS, width), F32),
            pltpu.VMEM((2, width // YS, width), F32),
            pltpu.VMEM((2, width, width), F32),
            pltpu.VMEM((lead, mats, width, width), F32),
            pltpu.SemaphoreType.DMA((5,)),
            pltpu.SemaphoreType.DMA((5,)),
            pltpu.SemaphoreType.DMA((3,)),
            pltpu.SemaphoreType.DMA((3,)),
            pltpu.SemaphoreType.DMA(((ITERS + 1) * NCHUNK,)),
            pltpu.SemaphoreType.DMA(((ITERS + 1) * NCHUNK,)),
            pltpu.SemaphoreType.DMA((ITERS + 1,)),
            pltpu.SemaphoreType.DMA((ITERS + 1,)),
            pltpu.SemaphoreType.DMA((12,)),
            pltpu.SemaphoreType.DMA((12,)),
            pltpu.SemaphoreType.DMA((8,)),
            pltpu.SemaphoreType.DMA((8,)),
        ],
        compiler_params=pltpu.CompilerParams(collective_id=0, has_side_effects=True),
    )(
        initial,
        source,
        mix_rate.reshape(1, width),
        fine_inverse,
        coarse_inverse,
        step_counts.reshape(groups, count // groups),
    )


def solution(mesh):
    return jax.shard_map(
        body,
        mesh=mesh,
        in_specs=(
            P("cell", None),
            P("tm", "cell", None),
            P(),
            P("tm", "cell", None, None),
            P("tm", "cell", None, None),
            P("cell"),
        ),
        out_specs=P("tm", "cell", None),
        check_vma=False,
    )
```

```python
import jax
import jax.numpy as jnp
from jax import lax
from jax.experimental import pallas as pl
from jax.experimental.pallas import tpu as pltpu
from jax.sharding import PartitionSpec as P

FINE_MAX = 8
ITERS = 2
FEWEST = 4
CLASSES = 5
MESH = pl.DeviceIdType.MESH
F32 = jnp.float32
BF16 = jnp.bfloat16
XS, YS, CORES = 4, 8, 2
NCHUNK = 8


def split(a):
    high = a.astype(BF16)
    low = (a - high.astype(F32)).astype(BF16)
    return jnp.concatenate([high, low], axis=1)


def put_weights(ref, matrix):
    width = matrix.shape[0]
    pair = split(matrix)
    ref[0:width, :] = pair
    ref[width : 2 * width, :] = pair


def halves(a):
    width = a.shape[1] // 2
    return a[:, :width] + a[:, width:]


def mul(a, weights):
    return halves(jnp.dot(split(a), weights[...], preferred_element_type=F32))


def mul_few(a, weights):
    high = a.astype(BF16)
    low = (a - high.astype(F32)).astype(BF16)
    size, width = a.shape
    both = jnp.dot(
        jnp.concatenate([high, low], axis=0),
        weights[0:width, :],
        preferred_element_type=F32,
    )
    return halves(both[:size] + both[size:])


def class_sums(onehot, cells):
    return halves(jnp.dot(onehot, split(cells), preferred_element_type=F32))


def pick(rows, counts):
    out = jnp.broadcast_to(rows[CLASSES : CLASSES + 1], counts.shape)
    for j in range(1, CLASSES):
        out = jnp.where(counts == float(FEWEST + j), rows[CLASSES + j : CLASSES + j + 1], out)
    return out


def cell_place():
    me = lax.axis_index("cell")
    return me // (CORES * YS), (me // CORES) % YS, me % CORES


def cell_index(x, y, core):
    return (x * YS + y) * CORES + core


def farthest_first(xs, ys, cores):
    x, y, core = cell_place()
    moves = [
        (min(dx, XS - dx) + min(dy, YS - dy), dx, dy, dc)
        for dx in range(xs)
        for dy in range(ys)
        for dc in range(cores)
        if dx or dy or dc
    ]
    moves.sort(reverse=True)
    return [
        cell_index((x + dx) % XS, (y + dy) % YS, (core + dc) % CORES) for _, dx, dy, dc in moves
    ]


def total_rows(a):
    return jnp.sum(a, axis=0, keepdims=True)


def arrived(ref, sem):
    pltpu.make_async_copy(ref, ref, sem).wait()


def kernel(
    initial, source, mix, fine, coarse, steps, out,
    wf, wc, wp, wk, wl, state, starts, off, shifted, counts, sums, weights_n, yinit,
    fine_p, coarse_p, begun, offy, sbuf, rbuf, many_s, many_r, zs, zr, ys, yr, fin, fin_p,
    kl, kd, ks, kx, kr, ky, kf, kg, kall,
    ssem, rsem, mssem, mrsem, zssem, zrsem, yssem, yrsem, kssem, krsem, pssem, prsem,
):
    lead, count, width = source.shape
    groups = fine.shape[1]
    every = 2 * groups
    per = count // groups
    tm = lax.axis_index("tm")
    last = lax.axis_size("tm") - 1
    x, y_at, core = cell_place()
    partner = cell_index(x, y_at, 1 - core)
    far_peers = farthest_first(XS, YS, 1)
    x_moves, y_moves = (2, 1, 3), (4, 3, 5, 2, 6, 1, 7)
    cells = count * lax.axis_size("cell")
    chunk = count // NCHUNK
    slab = width // YS
    used = 2 * CLASSES
    lead_core = core == 1

    barrier = pltpu.get_barrier_semaphore()

    def greet(peer):
        pl.semaphore_signal(barrier, inc=1, device_id={"cell": peer}, device_id_type=MESH)

    @pl.when(lead_core)
    def _():
        for peer in far_peers:
            greet(peer)

    @pl.when(jnp.logical_not(lead_core))
    def _():
        for d in x_moves:
            greet(cell_index((x + d) % XS, y_at, core))
        for d in y_moves:
            greet(cell_index(x, (y_at + d) % YS, core))

    greet(partner)
    behind = lax.rem(tm + last, last + 1)
    pl.semaphore_signal(barrier, inc=1, device_id={"tm": behind}, device_id_type=MESH)

    def rows(g):
        return pl.ds(g * per, per)

    def send(src, dst, ssem_one, rsem_one, peer):
        pltpu.make_async_remote_copy(
            src_ref=src,
            dst_ref=dst,
            send_sem=ssem_one,
            recv_sem=rsem_one,
            device_id={"cell": peer},
            device_id_type=MESH,
        ).start()

    rate = mix[...]
    keep = 1.0 - rate
    rate_down = jnp.broadcast_to(rate, (width, width)).T
    row_ids = lax.broadcasted_iota(jnp.int32, (16, width), 0)
    cell_row = row_ids[0:8] < CLASSES
    limits = jnp.where(
        row_ids < CLASSES, row_ids + FEWEST, jnp.where(row_ids < used, row_ids + FEWEST - CLASSES, 0)
    )
    shared = jnp.where(jnp.logical_and(row_ids >= CLASSES, row_ids < used), 1.0, 0.0).astype(F32)

    def padded(a):
        return jnp.concatenate([a, jnp.zeros_like(a)], axis=0)

    numbers = []
    for g in range(groups):
        for l in range(lead):
            put_weights(wf.at[l, g], fine[l, g])
            put_weights(wc.at[l, g], coarse[l, g])
        line = steps[g : g + 1, :]
        hot = jnp.where(
            jnp.logical_and(line == row_ids[0:8] + FEWEST, cell_row), 1.0, 0.0
        ).astype(F32)
        onehot = hot.astype(BF16)
        number = jnp.broadcast_to(jnp.sum(hot, axis=1, keepdims=True), (8, width))
        numbers.append(number)
        weights_n[g] = (padded(number) + shared) * rate
        counts[g] = jnp.broadcast_to(line.astype(F32), (per, width)).T
        yinit[g] = padded(class_sums(onehot, initial[rows(g)]))
        for l in range(lead):
            sums[l, g] = padded(class_sums(onehot, source[l, rows(g)]))
            offy[l, g] = mul_few(sums[l, g], wc.at[l, g])
        begun[0, g] = yinit[g]
        begun[1, g] = mul_few(yinit[g], wc.at[0, g]) + offy[0, g]
        ys[0, g] = mul_few(begun[1, g], wc.at[1, g]) + offy[1, g]

    def bulk_setup():
        for g in range(groups):
            put_weights(wp.at[g], mul(coarse[0, g], wc.at[1, g]))
            for l in range(lead):
                off[l, rows(g)] = mul(source[l, rows(g)], wc.at[l, g])
            shifted[rows(g)] = mul(off[0, rows(g)], wc.at[1, g]) + off[1, rows(g)]

    def condense():
        over = 1.0 / cells
        for l in range(lead):
            for g in range(groups):
                six, seven = numbers[g][2:3] * over, (numbers[g][3:4] + numbers[g][4:5]) * over
                effect = rate_down * fine[l, g]
                terms = [(six + seven) * effect, seven * effect, six * effect, None]
                for d in range(4):
                    terms.append(effect * (per * over))
                    if d < 3:
                        effect = mul(effect * keep, wf.at[l, g])
                    if d == 0:
                        terms[2] += seven * effect
                for i, term in enumerate(terms):
                    if term is None:
                        kl[l, i] = jnp.zeros((width, width), F32)
                    elif g == 0:
                        kl[l, i] = term
                    else:
                        kl[l, i] += term

    @pl.when(tm == 0)
    def _():
        for k in range(ITERS + 1):
            zr[k] = initial[...]

    def k_sems(stage, b):
        return kssem.at[stage * 2 + b], krsem.at[stage * 2 + b]

    def batch(b):
        return pl.ds(b * XS, XS)

    def pair_reduce_start(b):
        send(kl.at[1 - core, batch(b)], kd.at[batch(b)], *k_sems(0, b), partner)

    def x_reduce_start(b):
        arrived(kd.at[batch(b)], k_sems(0, b)[1])
        for i in range(XS):
            ks[b * XS + i] = kl[core, b * XS + i] + kd[b * XS + i]
        for slot, dx in enumerate(x_moves):
            to = (x + dx) % XS
            send(ks.at[b * XS + to], kx.at[b, slot], *k_sems(1, b), cell_index(to, y_at, core))

    def y_reduce_start(b):
        arrived(kx.at[b], k_sems(1, b)[1])
        kr[b] = ks[b * XS + x] + kx[b, 0] + kx[b, 1] + kx[b, 2]
        for slot, dy in enumerate(y_moves):
            to = (y_at + dy) % YS
            part = pl.ds(pl.multiple_of(to * slab, slab), slab)
            send(kr.at[b, part], ky.at[b, slot], *k_sems(2, b), cell_index(x, to, core))

    def y_gather_start(b):
        arrived(ky.at[b], k_sems(2, b)[1])
        part = pl.ds(pl.multiple_of(y_at * slab, slab), slab)
        piece = kr[b, part] + jnp.sum(ky[b], axis=0)
        kf[b] = piece
        kg[b, part] = piece
        for dy in y_moves:
            send(kf.at[b], kg.at[b, part], *k_sems(3, b), cell_index(x, (y_at + dy) % YS, core))

    def x_gather_start(b):
        arrived(ky.at[b], k_sems(3, b)[1])
        kall[core, b * XS + x] = kg[b]
        for dx in x_moves:
            send(
                kg.at[b], kall.at[core, b * XS + x], *k_sems(4, b),
                cell_index((x + dx) % XS, y_at, core),
            )

    def x_gather_done(b):
        arrived(kx.at[b], k_sems(4, b)[1])

    def pair_gather_start(b):
        x_gather_done(b)
        send(kall.at[core, batch(b)], kall.at[core, batch(b)], *k_sems(5, b), partner)

    def k_finish(b):
        arrived(kall.at[1 - core, batch(b)], k_sems(5, b)[1])
        for l in range(lead):
            for i in range(XS):
                if b or i < 2:
                    put_weights(wk.at[l, b * XS + i], kall[l, b * XS + i])
            if b == 0:
                put_weights(wk.at[l, 2], kall[l, 2] + mul(kall[l, 0], wk.at[l, 1]))
            else:
                solved = []
                for d in range(XS):
                    term = kall[l, XS + d]
                    for e, earlier in enumerate(solved):
                        term = term + mul(earlier, wk.at[l, XS + d - 1 - e])
                    solved.append(term)
                    wl[l, d] = split(term)

    def hop(k, j):
        part = pl.ds(j * chunk, chunk)
        return pltpu.make_async_remote_copy(
            src_ref=zs.at[k, part],
            dst_ref=zr.at[k, part],
            send_sem=zssem.at[k * NCHUNK + j],
            recv_sem=zrsem.at[k * NCHUNK + j],
            device_id={"tm": lax.rem(tm + 1, last + 1)},
            device_id_type=MESH,
        )

    def bulk_chain(k):
        for j in range(NCHUNK):
            part = pl.ds(j * chunk, chunk)

            @pl.when(tm > 0)
            def _():
                hop(k, j).wait_recv()

            zs[k, part] = mul(zr[k, part], wp.at[j * chunk // per]) + shifted[part]

            @pl.when(tm < last)
            def _():
                hop(k, j).start()

    def bulk_begin(it):
        for g in range(groups):
            first = zr[it, rows(g)]
            second = mul(first, wc.at[0, g]) + off[0, rows(g)]
            starts[1, rows(g)] = second
            state[0, rows(g)] = first
            state[1, rows(g)] = second

    def fine_cells(m):
        for l in range(lead):
            for g in range(groups):
                old = state[l, rows(g)]
                new = mul(old * keep + source[l, rows(g)], wf.at[l, g])
                if m >= FEWEST:
                    new = jnp.where(counts[g] > float(m), new, old)
                state[l, rows(g)] = new

    def bulk_offsets(it):
        for g in range(groups):
            for l in range(lead):
                begin = zr[it, rows(g)] if l == 0 else starts[1, rows(g)]
                off[l, rows(g)] = state[l, rows(g)] - mul(begin, wc.at[l, g])
            shifted[rows(g)] = mul(off[0, rows(g)], wc.at[1, g]) + off[1, rows(g)]

    def bulk_result():
        for g in range(groups):
            state[0, rows(g)] = mul(zr[ITERS, rows(g)], wc.at[0, g]) + off[0, rows(g)]

    def result(rows_of):
        for g in range(groups):
            out[0, rows(g)] = state[0, rows(g)] + pick(rows_of(0, g), counts[g])
            out[1, rows(g)] = zs[ITERS, rows(g)] + pick(rows_of(1, g), counts[g])

    def drain_common():
        for b in range(2):
            for stage, ref in enumerate((kd.at[batch(b)], kx.at[b], ky.at[b], ky.at[b], kx.at[b])):
                arrived(ref, k_sems(stage, b)[0])

        @pl.when(tm < last)
        def _():
            for k in range(ITERS + 1):
                for j in range(NCHUNK):
                    hop(k, j).wait_send()

    own_groups, partner_groups = pl.ds(0, groups), pl.ds(groups, groups)

    def shared_copies():
        def both(ref):
            return ref.at[own_groups], ref.at[partner_groups]

        return [
            both(begun.at[0]), both(begun.at[1]), both(ys.at[0]),
            both(weights_n), both(yinit), both(sums.at[0]), both(sums.at[1]),
            both(offy.at[0]), both(offy.at[1]),
            (coarse, coarse_p), (fine, fine_p),
        ]

    @pl.when(jnp.logical_not(lead_core))
    def _():
        pl.semaphore_wait(barrier, len(x_moves) + len(y_moves) + 2)
        for i, (src, dst) in enumerate(shared_copies()):
            send(src, dst, pssem.at[i], prsem.at[i], partner)
        condense()
        pair_reduce_start(0)
        pair_reduce_start(1)
        bulk_setup()
        x_reduce_start(0)
        x_reduce_start(1)
        y_reduce_start(0)
        bulk_chain(0)
        bulk_begin(0)
        y_gather_start(0)
        for m in range(4):
            fine_cells(m)
        y_reduce_start(1)
        x_gather_start(0)
        for m in range(4, FINE_MAX):
            fine_cells(m)
        y_gather_start(1)
        pair_gather_start(0)
        bulk_offsets(0)
        x_gather_start(1)
        bulk_chain(1)
        bulk_begin(1)
        pair_gather_start(1)
        for m in range(FINE_MAX):
            fine_cells(m)
        bulk_offsets(1)
        bulk_chain(2)
        bulk_result()
        arrived(fin_p, prsem.at[11])
        result(lambda l, g: fin_p[l, g])
        for i, (src, _) in enumerate(shared_copies()):
            arrived(src, pssem.at[i])
        for b in range(2):
            arrived(kd.at[batch(b)], k_sems(5, b)[0])
        drain_common()

    @pl.when(lead_core)
    def _():
        bulk_setup()
        condense()
        pl.semaphore_wait(barrier, len(far_peers) + 2)
        pair_reduce_start(0)
        pair_reduce_start(1)
        def await_copies(first, end):
            for i, (_, dst) in enumerate(shared_copies()):
                if first <= i < end:
                    arrived(dst, prsem.at[i])

        def prepare():
            await_copies(3, 10)
            for g in range(groups):
                for l in range(lead):
                    put_weights(wc.at[l, groups + g], coarse_p[l, g])
                put_weights(wp.at[groups + g], mul(coarse_p[0, g], wc.at[1, groups + g]))

        await_copies(0, 3)

        each = [(l, g) for l in range(lead) for g in range(every)]
        used_rows = pl.ds(0, used)

        def row_hop(k):
            return pltpu.make_async_remote_copy(
                src_ref=ys.at[k, :, used_rows],
                dst_ref=yr.at[k, :, used_rows],
                send_sem=yssem.at[k],
                recv_sem=yrsem.at[k],
                device_id={"tm": lax.rem(tm + 1, last + 1)},
                device_id_type=MESH,
            )

        def row_chain(k):
            step = [mul_few(offy[0, g], wc.at[1, g]) + offy[1, g] for g in range(every)]

            @pl.when(tm > 0)
            def _():
                row_hop(k).wait_recv()

            for g in range(every):
                ys[k, g] = mul_few(yr[k, g], wp.at[g]) + step[g]

            @pl.when(tm < last)
            def _():
                row_hop(k).start()

        def row_begin(k):
            y = {}
            for g in range(every):
                y[0, g] = yr[k, g]
                y[1, g] = mul_few(yr[k, g], wc.at[0, g]) + offy[0, g]
            for l, g in each:
                begun[l, g] = y[l, g]
            return y

        def row_coarse():
            for l, g in each:
                begun[l, g] = mul_few(begun[l, g], wc.at[l, g])

        def row_offsets(y):
            for l, g in each:
                offy[l, g] = y[l, g] - begun[l, g]

        def exchange_one(turn, own, work):
            sbuf[turn] = own
            for slot, peer in enumerate(far_peers):
                send(sbuf.at[turn], rbuf.at[turn, slot], ssem.at[turn], rsem.at[turn], peer)
            work()
            arrived(rbuf.at[turn], rsem.at[turn])
            return (own + jnp.sum(rbuf[turn], axis=0)) * (1.0 / cells)

        def exchange_many(turn, own, work):
            part = pl.ds(0, own.shape[0])
            many_s[turn, part] = own
            for slot, peer in enumerate(far_peers):
                send(
                    many_s.at[turn, part], many_r.at[turn, slot, part],
                    mssem.at[turn], mrsem.at[turn], peer,
                )
            work()
            arrived(many_r.at[turn, :, part], mrsem.at[turn])
            return (own + jnp.sum(many_r[turn, :, part], axis=0)) * (1.0 / cells)

        def partial(y, l):
            return total_rows(jnp.where(cell_row, sum(y[l, g][0:8] for g in range(every)), 0.0))

        def advance(y, m, average):
            made = {}
            for l, g in each:
                old = y[l, g]
                size = old.shape[0]
                fed = old * keep + sums[l, g, 0:size]
                if average is not None:
                    fed = fed + weights_n[g] * average[l]
                new = mul_few(fed, wf.at[l, g])
                made[l, g] = jnp.where(limits[0:size] > m, new, old) if m >= FEWEST else new
            return made

        def through(row, l, i):
            return mul_few(jnp.broadcast_to(row, (8, width)), wk.at[l, i])[0:1]

        def late(y, turn, work):
            free = [y]
            for m in (5, 6):
                tops = {k: v[0:8] for k, v in free[-1].items()}
                free.append(advance(tops, m, None))
            own = jnp.concatenate([partial(f, l) for l in range(lead) for f in free], axis=0)
            got = exchange_many(turn, own, work)
            fifth = [got[3 * l : 3 * l + 1] for l in range(lead)]
            y = advance(y, 5, fifth)
            sixth, seventh = [], []
            for l in range(lead):
                free_sixth = got[3 * l + 1 : 3 * l + 2]
                sixth.append(free_sixth + through(fifth[l], l, 0))
                seventh.append(
                    got[3 * l + 2 : 3 * l + 3] + through(fifth[l], l, 2) + through(free_sixth, l, 1)
                )
            y = advance(y, 6, sixth)
            return advance(y, 7, seventh)

        @pl.when(tm == 0)
        def _():
            row_hop(0).start()

        @pl.when(tm > 0)
        def _():
            prepare()
            row_chain(0)
            row_begin(0)

        y = {(l, g): begun[l, g] for l, g in each}

        def beside(m):
            def work():
                if m == 0:
                    @pl.when(tm == 0)
                    def _():
                        prepare()
                        for k in range(ITERS + 1):
                            yr[k] = yinit[...]

                    await_copies(10, 11)
                    for g in range(groups):
                        for l in range(lead):
                            put_weights(wf.at[l, groups + g], fine_p[l, g])
                    x_reduce_start(0)
                    row_coarse()
                elif m == 1:
                    y_reduce_start(0)
                    x_reduce_start(1)
                    bulk_chain(0)
                elif m == 2:
                    y_gather_start(0)
                    bulk_begin(0)
                    for i in range(4):
                        fine_cells(i)
                elif m == 3:
                    x_gather_start(0)
                    y_reduce_start(1)
                    for i in range(4, FINE_MAX):
                        fine_cells(i)
                elif m == 4:
                    y_gather_start(1)
                    x_gather_done(0)
                    bulk_offsets(0)
                else:
                    x_gather_start(1)
                    bulk_chain(1)
                    k_finish(0)

            return work

        for m in range(5):
            own = jnp.concatenate([partial(y, l) for l in range(lead)], axis=0)
            average = exchange_one(m, own, beside(m))
            y = advance(y, m, [average[l : l + 1] for l in range(lead)])
        row_offsets(late(y, 0, beside(5)))
        row_chain(1)

        y = row_begin(1)
        free = [{k: v[0:8] for k, v in y.items()}]
        for m in range(4):
            free.append(advance(free[-1], m, None))
        own = jnp.concatenate([partial(f, l) for l in range(lead) for f in free], axis=0)

        def work():
            row_coarse()
            bulk_begin(1)
            for m in range(FINE_MAX):
                fine_cells(m)
            x_gather_done(1)
            k_finish(1)

        got = exchange_many(1, own, work)
        averages = [[got[5 * l + m : 5 * l + m + 1] for m in range(5)] for l in range(lead)]
        for l in range(lead):
            free_rows = jnp.concatenate(averages[l] + [jnp.zeros((3, width), F32)], axis=0)
            for d in range(1, 5):
                fed = mul_few(free_rows, wl.at[l, d - 1])
                for m in range(d, 5):
                    averages[l][m] = averages[l][m] + fed[m - d : m - d + 1]
        for m in range(5):
            y = advance(y, m, [averages[l][m] for l in range(lead)])

        def work():
            bulk_offsets(1)
            bulk_chain(2)
            bulk_result()

        row_offsets(late(y, 2, work))
        row_chain(2)
        for g in range(every):
            fin[0, g] = mul_few(yr[ITERS, g], wc.at[0, g]) + offy[0, g]
            fin[1, g] = ys[ITERS, g]
        for l in range(lead):
            send(fin.at[l, partner_groups], fin_p.at[l], pssem.at[11 + l], prsem.at[11], partner)
        result(lambda l, g: fin[l, g])

        for turn in range(5):
            arrived(rbuf.at[turn], ssem.at[turn])
        for turn, size in ((0, 6), (1, 10), (2, 6)):
            arrived(many_r.at[turn, :, pl.ds(0, size)], mssem.at[turn])
        for l in range(lead):
            arrived(fin_p.at[l], pssem.at[11 + l])
        drain_common()

        @pl.when(tm < last)
        def _():
            for k in range(ITERS + 1):
                row_hop(k).wait_send()


def body(initial, source, mix_rate, fine_inverse, coarse_inverse, step_counts):
    lead, count, width = source.shape
    groups = fine_inverse.shape[1]
    every = 2 * groups
    far = XS * YS - 1
    mats = 2 * XS
    vmem = pl.BlockSpec(memory_space=pltpu.VMEM)
    return pl.pallas_call(
        kernel,
        out_shape=jax.ShapeDtypeStruct(source.shape, F32),
        in_specs=[vmem] * 6,
        out_specs=vmem,
        scratch_shapes=[
            pltpu.VMEM((lead, every, 2 * width, 2 * width), BF16),
            pltpu.VMEM((lead, every, 2 * width, 2 * width), BF16),
            pltpu.VMEM((every, 2 * width, 2 * width), BF16),
            pltpu.VMEM((lead, mats, 2 * width, 2 * width), BF16),
            pltpu.VMEM((lead, XS, width, 2 * width), BF16),
            pltpu.VMEM((lead, count, width), F32),
            pltpu.VMEM((lead, count, width), F32),
            pltpu.VMEM((lead, count, width), F32),
            pltpu.VMEM((count, width), F32),
            pltpu.VMEM((groups, count // groups, width), F32),
            pltpu.VMEM((lead, every, 16, width), F32),
            pltpu.VMEM((every, 16, width), F32),
            pltpu.VMEM((every, 16, width), F32),
            pltpu.VMEM((lead, groups, width, width), F32),
            pltpu.VMEM((lead, groups, width, width), F32),
            pltpu.VMEM((lead, every, 16, width), F32),
            pltpu.VMEM((lead, every, 16, width), F32),
            pltpu.VMEM((5, lead, width), F32),
            pltpu.VMEM((5, far, lead, width), F32),
            pltpu.VMEM((3, 16, width), F32),
            pltpu.VMEM((3, far, 16, width), F32),
            pltpu.VMEM((ITERS + 1, count, width), F32),
            pltpu.VMEM((ITERS + 1, count, width), F32),
            pltpu.VMEM((ITERS + 1, every, 16, width), F32),
            pltpu.VMEM((ITERS + 1, every, 16, width), F32),
            pltpu.VMEM((lead, every, 16, width), F32),
            pltpu.VMEM((lead, groups, 16, width), F32),
            pltpu.VMEM((lead, mats, width, width), F32),
            pltpu.VMEM((mats, width, width), F32),
            pltpu.VMEM((mats, width, width), F32),
            pltpu.VMEM((2, XS - 1, width, width), F32),
            pltpu.VMEM((2, width, width), F32),
            pltpu.VMEM((2, YS - 1, width // YS, width), F32),
            pltpu.VMEM((2, width // YS, width), F32),
            pltpu.VMEM((2, width, width), F32),
            pltpu.VMEM((lead, mats, width, width), F32),
            pltpu.SemaphoreType.DMA((5,)),
            pltpu.SemaphoreType.DMA((5,)),
            pltpu.SemaphoreType.DMA((3,)),
            pltpu.SemaphoreType.DMA((3,)),
            pltpu.SemaphoreType.DMA(((ITERS + 1) * NCHUNK,)),
            pltpu.SemaphoreType.DMA(((ITERS + 1) * NCHUNK,)),
            pltpu.SemaphoreType.DMA((ITERS + 1,)),
            pltpu.SemaphoreType.DMA((ITERS + 1,)),
            pltpu.SemaphoreType.DMA((12,)),
            pltpu.SemaphoreType.DMA((12,)),
            pltpu.SemaphoreType.DMA((13,)),
            pltpu.SemaphoreType.DMA((13,)),
        ],
        compiler_params=pltpu.CompilerParams(collective_id=0, has_side_effects=True),
    )(
        initial,
        source,
        mix_rate.reshape(1, width),
        fine_inverse,
        coarse_inverse,
        step_counts.reshape(groups, count // groups),
    )


def solution(mesh):
    return jax.shard_map(
        body,
        mesh=mesh,
        in_specs=(
            P("cell", None),
            P("tm", "cell", None),
            P(),
            P("tm", "cell", None, None),
            P("tm", "cell", None, None),
            P("cell"),
        ),
        out_specs=P("tm", "cell", None),
        check_vma=False,
    )
```

```python
import jax
import jax.numpy as jnp
from jax import lax
from jax.experimental import pallas as pl
from jax.experimental.pallas import tpu as pltpu
from jax.sharding import PartitionSpec as P

FINE_MAX = 8
ITERS = 2
FEWEST = 4
CLASSES = 5
MESH = pl.DeviceIdType.MESH
F32 = jnp.float32
BF16 = jnp.bfloat16
XS, YS, CORES = 4, 8, 2
NCHUNK = 8


def split(a):
    high = a.astype(BF16)
    low = (a - high.astype(F32)).astype(BF16)
    return jnp.concatenate([high, low], axis=1)


def put_weights(ref, matrix):
    width = matrix.shape[0]
    pair = split(matrix)
    ref[0:width, :] = pair
    ref[width : 2 * width, :] = pair


def halves(a):
    width = a.shape[1] // 2
    return a[:, :width] + a[:, width:]


def mul(a, weights):
    return halves(jnp.dot(split(a), weights[...], preferred_element_type=F32))


def mul_few(a, weights):
    high = a.astype(BF16)
    low = (a - high.astype(F32)).astype(BF16)
    size, width = a.shape
    both = jnp.dot(
        jnp.concatenate([high, low], axis=0),
        weights[0:width, :],
        preferred_element_type=F32,
    )
    return halves(both[:size] + both[size:])


def class_sums(onehot, cells):
    return halves(jnp.dot(onehot, split(cells), preferred_element_type=F32))


def pick(rows, counts):
    out = jnp.broadcast_to(rows[CLASSES : CLASSES + 1], counts.shape)
    for j in range(1, CLASSES):
        out = jnp.where(counts == float(FEWEST + j), rows[CLASSES + j : CLASSES + j + 1], out)
    return out


def cell_place():
    me = lax.axis_index("cell")
    return me // (CORES * YS), (me // CORES) % YS, me % CORES


def cell_index(x, y, core):
    return (x * YS + y) * CORES + core


def farthest_first(xs, ys, cores):
    x, y, core = cell_place()
    moves = [
        (min(dx, XS - dx) + min(dy, YS - dy), dx, dy, dc)
        for dx in range(xs)
        for dy in range(ys)
        for dc in range(cores)
        if dx or dy or dc
    ]
    moves.sort(reverse=True)
    return [
        cell_index((x + dx) % XS, (y + dy) % YS, (core + dc) % CORES) for _, dx, dy, dc in moves
    ]


def total_rows(a):
    return jnp.sum(a, axis=0, keepdims=True)


def arrived(ref, sem):
    pltpu.make_async_copy(ref, ref, sem).wait()


def kernel(
    initial, source, mix, fine, coarse, steps, out,
    wf, wc, wp, wk, wl, state, starts, off, shifted, counts, sums, weights_n, yinit,
    fine_p, coarse_p, begun, offy, sbuf, rbuf, many_s, many_r, zs, zr, ys, yr, fin, fin_p,
    kl, kd, ks, kx, kr, ky, kf, kg, kall,
    ssem, rsem, mssem, mrsem, zssem, zrsem, yssem, yrsem, kssem, krsem, pssem, prsem,
):
    lead, count, width = source.shape
    groups = fine.shape[1]
    every = 2 * groups
    per = count // groups
    tm = lax.axis_index("tm")
    last = lax.axis_size("tm") - 1
    x, y_at, core = cell_place()
    partner = cell_index(x, y_at, 1 - core)
    far_peers = farthest_first(XS, YS, 1)
    x_moves, y_moves = (2, 1, 3), (4, 3, 5, 2, 6, 1, 7)
    cells = count * lax.axis_size("cell")
    chunk = count // NCHUNK
    slab = width // YS
    used = 2 * CLASSES
    lead_core = core == 1

    barrier = pltpu.get_barrier_semaphore()

    def greet(peer):
        pl.semaphore_signal(barrier, inc=1, device_id={"cell": peer}, device_id_type=MESH)

    @pl.when(lead_core)
    def _():
        for peer in far_peers:
            greet(peer)

    @pl.when(jnp.logical_not(lead_core))
    def _():
        for d in x_moves:
            greet(cell_index((x + d) % XS, y_at, core))
        for d in y_moves:
            greet(cell_index(x, (y_at + d) % YS, core))

    greet(partner)
    behind = lax.rem(tm + last, last + 1)
    pl.semaphore_signal(barrier, inc=1, device_id={"tm": behind}, device_id_type=MESH)

    def rows(g):
        return pl.ds(g * per, per)

    def send(src, dst, ssem_one, rsem_one, peer):
        pltpu.make_async_remote_copy(
            src_ref=src,
            dst_ref=dst,
            send_sem=ssem_one,
            recv_sem=rsem_one,
            device_id={"cell": peer},
            device_id_type=MESH,
        ).start()

    rate = mix[...]
    keep = 1.0 - rate
    rate_down = jnp.broadcast_to(rate, (width, width)).T
    row_ids = lax.broadcasted_iota(jnp.int32, (16, width), 0)
    cell_row = row_ids[0:8] < CLASSES
    limits = jnp.where(
        row_ids < CLASSES, row_ids + FEWEST, jnp.where(row_ids < used, row_ids + FEWEST - CLASSES, 0)
    )
    shared = jnp.where(jnp.logical_and(row_ids >= CLASSES, row_ids < used), 1.0, 0.0).astype(F32)

    def padded(a):
        return jnp.concatenate([a, jnp.zeros_like(a)], axis=0)

    numbers = []
    for g in range(groups):
        for l in range(lead):
            put_weights(wf.at[l, g], fine[l, g])
            put_weights(wc.at[l, g], coarse[l, g])
        line = steps[g : g + 1, :]
        hot = jnp.where(
            jnp.logical_and(line == row_ids[0:8] + FEWEST, cell_row), 1.0, 0.0
        ).astype(F32)
        onehot = hot.astype(BF16)
        number = jnp.broadcast_to(jnp.sum(hot, axis=1, keepdims=True), (8, width))
        numbers.append(number)
        weights_n[g] = (padded(number) + shared) * rate
        counts[g] = jnp.broadcast_to(line.astype(F32), (per, width)).T
        yinit[g] = padded(class_sums(onehot, initial[rows(g)]))
        for l in range(lead):
            sums[l, g] = padded(class_sums(onehot, source[l, rows(g)]))
            offy[l, g] = mul_few(sums[l, g], wc.at[l, g])
        begun[0, g] = yinit[g]
        begun[1, g] = mul_few(yinit[g], wc.at[0, g]) + offy[0, g]
        ys[0, g] = mul_few(begun[1, g], wc.at[1, g]) + offy[1, g]

    def bulk_setup():
        for g in range(groups):
            put_weights(wp.at[g], mul(coarse[0, g], wc.at[1, g]))
            for l in range(lead):
                off[l, rows(g)] = mul(source[l, rows(g)], wc.at[l, g])
            shifted[rows(g)] = mul(off[0, rows(g)], wc.at[1, g]) + off[1, rows(g)]

    def condense():
        over = 1.0 / cells
        for l in range(lead):
            for g in range(groups):
                six, seven = numbers[g][2:3] * over, (numbers[g][3:4] + numbers[g][4:5]) * over
                effect = rate_down * fine[l, g]
                terms = [(six + seven) * effect, seven * effect, six * effect, None]
                for d in range(4):
                    terms.append(effect * (per * over))
                    if d < 3:
                        effect = mul(effect * keep, wf.at[l, g])
                    if d == 0:
                        terms[2] += seven * effect
                for i, term in enumerate(terms):
                    if term is None:
                        kl[l, i] = jnp.zeros((width, width), F32)
                    elif g == 0:
                        kl[l, i] = term
                    else:
                        kl[l, i] += term

    @pl.when(tm == 0)
    def _():
        for k in range(ITERS + 1):
            zr[k] = initial[...]

    def k_sems(stage, b):
        return kssem.at[stage * 2 + b], krsem.at[stage * 2 + b]

    def batch(b):
        return pl.ds(b * XS, XS)

    def pair_reduce_start(b):
        send(kl.at[1 - core, batch(b)], kd.at[batch(b)], *k_sems(0, b), partner)

    def x_reduce_start(b):
        arrived(kd.at[batch(b)], k_sems(0, b)[1])
        for i in range(XS):
            ks[b * XS + i] = kl[core, b * XS + i] + kd[b * XS + i]
        for slot, dx in enumerate(x_moves):
            to = (x + dx) % XS
            send(ks.at[b * XS + to], kx.at[b, slot], *k_sems(1, b), cell_index(to, y_at, core))

    def y_reduce_start(b):
        arrived(kx.at[b], k_sems(1, b)[1])
        kr[b] = ks[b * XS + x] + kx[b, 0] + kx[b, 1] + kx[b, 2]
        for slot, dy in enumerate(y_moves):
            to = (y_at + dy) % YS
            part = pl.ds(pl.multiple_of(to * slab, slab), slab)
            send(kr.at[b, part], ky.at[b, slot], *k_sems(2, b), cell_index(x, to, core))

    def y_gather_start(b):
        arrived(ky.at[b], k_sems(2, b)[1])
        part = pl.ds(pl.multiple_of(y_at * slab, slab), slab)
        piece = kr[b, part] + jnp.sum(ky[b], axis=0)
        kf[b] = piece
        kg[b, part] = piece
        for dy in y_moves:
            send(kf.at[b], kg.at[b, part], *k_sems(3, b), cell_index(x, (y_at + dy) % YS, core))

    def x_gather_start(b):
        arrived(ky.at[b], k_sems(3, b)[1])
        kall[core, b * XS + x] = kg[b]
        for dx in x_moves:
            send(
                kg.at[b], kall.at[core, b * XS + x], *k_sems(4, b),
                cell_index((x + dx) % XS, y_at, core),
            )

    def x_gather_done(b):
        arrived(kx.at[b], k_sems(4, b)[1])

    def pair_gather_start(b):
        x_gather_done(b)
        send(kall.at[core, batch(b)], kall.at[core, batch(b)], *k_sems(5, b), partner)

    def k_finish(b):
        arrived(kall.at[1 - core, batch(b)], k_sems(5, b)[1])
        for l in range(lead):
            for i in range(XS):
                if b or i < 2:
                    put_weights(wk.at[l, b * XS + i], kall[l, b * XS + i])
            if b == 0:
                put_weights(wk.at[l, 2], kall[l, 2] + mul(kall[l, 0], wk.at[l, 1]))
            else:
                solved = []
                for d in range(XS):
                    term = kall[l, XS + d]
                    for e, earlier in enumerate(solved):
                        term = term + mul(earlier, wk.at[l, XS + d - 1 - e])
                    solved.append(term)
                    wl[l, d] = split(term)

    def hop(k, j):
        part = pl.ds(j * chunk, chunk)
        return pltpu.make_async_remote_copy(
            src_ref=zs.at[k, part],
            dst_ref=zr.at[k, part],
            send_sem=zssem.at[k * NCHUNK + j],
            recv_sem=zrsem.at[k * NCHUNK + j],
            device_id={"tm": lax.rem(tm + 1, last + 1)},
            device_id_type=MESH,
        )

    def bulk_chain(k):
        for j in range(NCHUNK):
            part = pl.ds(j * chunk, chunk)

            @pl.when(tm > 0)
            def _():
                hop(k, j).wait_recv()

            zs[k, part] = mul(zr[k, part], wp.at[j * chunk // per]) + shifted[part]

            @pl.when(tm < last)
            def _():
                hop(k, j).start()

    def bulk_begin(it):
        for g in range(groups):
            first = zr[it, rows(g)]
            second = mul(first, wc.at[0, g]) + off[0, rows(g)]
            starts[1, rows(g)] = second
            state[0, rows(g)] = first
            state[1, rows(g)] = second

    def fine_cells(m):
        for l in range(lead):
            for g in range(groups):
                old = state[l, rows(g)]
                new = mul(old * keep + source[l, rows(g)], wf.at[l, g])
                if m >= FEWEST:
                    new = jnp.where(counts[g] > float(m), new, old)
                state[l, rows(g)] = new

    def bulk_offsets(it):
        for g in range(groups):
            for l in range(lead):
                begin = zr[it, rows(g)] if l == 0 else starts[1, rows(g)]
                off[l, rows(g)] = state[l, rows(g)] - mul(begin, wc.at[l, g])
            shifted[rows(g)] = mul(off[0, rows(g)], wc.at[1, g]) + off[1, rows(g)]

    def bulk_result():
        for g in range(groups):
            state[0, rows(g)] = mul(zr[ITERS, rows(g)], wc.at[0, g]) + off[0, rows(g)]

    def result(rows_of):
        for g in range(groups):
            out[0, rows(g)] = state[0, rows(g)] + pick(rows_of(0, g), counts[g])
            out[1, rows(g)] = zs[ITERS, rows(g)] + pick(rows_of(1, g), counts[g])

    def drain_common():
        for b in range(2):
            for stage, ref in enumerate((kd.at[batch(b)], kx.at[b], ky.at[b], ky.at[b], kx.at[b])):
                arrived(ref, k_sems(stage, b)[0])

        @pl.when(tm < last)
        def _():
            for k in range(ITERS + 1):
                for j in range(NCHUNK):
                    hop(k, j).wait_send()

    own_groups, partner_groups = pl.ds(0, groups), pl.ds(groups, groups)

    def shared_copies():
        def both(ref):
            return ref.at[own_groups], ref.at[partner_groups]

        return [
            both(begun.at[0]), both(begun.at[1]), both(ys.at[0]),
            both(weights_n), both(yinit), both(sums.at[0]), both(sums.at[1]),
            both(offy.at[0]), both(offy.at[1]),
            (coarse, coarse_p), (fine, fine_p),
        ]

    @pl.when(jnp.logical_not(lead_core))
    def _():
        pl.semaphore_wait(barrier, len(x_moves) + len(y_moves) + 2)
        for i, (src, dst) in enumerate(shared_copies()):
            send(src, dst, pssem.at[i], prsem.at[i], partner)
        condense()
        pair_reduce_start(0)
        pair_reduce_start(1)
        bulk_setup()
        x_reduce_start(0)
        x_reduce_start(1)
        y_reduce_start(0)
        bulk_chain(0)
        bulk_begin(0)
        y_gather_start(0)
        for m in range(4):
            fine_cells(m)
        y_reduce_start(1)
        x_gather_start(0)
        for m in range(4, FINE_MAX):
            fine_cells(m)
        y_gather_start(1)
        pair_gather_start(0)
        bulk_offsets(0)
        x_gather_start(1)
        bulk_chain(1)
        bulk_begin(1)
        pair_gather_start(1)
        for m in range(FINE_MAX):
            fine_cells(m)
        bulk_offsets(1)
        bulk_chain(2)
        bulk_result()
        arrived(fin_p, prsem.at[11])
        result(lambda l, g: fin_p[l, g])
        for i, (src, _) in enumerate(shared_copies()):
            arrived(src, pssem.at[i])
        for b in range(2):
            arrived(kd.at[batch(b)], k_sems(5, b)[0])
        drain_common()

    @pl.when(lead_core)
    def _():
        bulk_setup()
        condense()
        pl.semaphore_wait(barrier, len(far_peers) + 2)
        pair_reduce_start(0)
        pair_reduce_start(1)
        def await_copies(first, end):
            for i, (_, dst) in enumerate(shared_copies()):
                if first <= i < end:
                    arrived(dst, prsem.at[i])

        def prepare():
            await_copies(3, 10)
            for g in range(groups):
                for l in range(lead):
                    put_weights(wc.at[l, groups + g], coarse_p[l, g])
                put_weights(wp.at[groups + g], mul(coarse_p[0, g], wc.at[1, groups + g]))

        await_copies(0, 3)

        each = [(l, g) for l in range(lead) for g in range(every)]
        used_rows = pl.ds(0, used)

        def row_hop(k):
            return pltpu.make_async_remote_copy(
                src_ref=ys.at[k, :, used_rows],
                dst_ref=yr.at[k, :, used_rows],
                send_sem=yssem.at[k],
                recv_sem=yrsem.at[k],
                device_id={"tm": lax.rem(tm + 1, last + 1)},
                device_id_type=MESH,
            )

        def row_chain(k):
            step = [mul_few(offy[0, g], wc.at[1, g]) + offy[1, g] for g in range(every)]

            @pl.when(tm > 0)
            def _():
                row_hop(k).wait_recv()

            for g in range(every):
                ys[k, g] = mul_few(yr[k, g], wp.at[g]) + step[g]

            @pl.when(tm < last)
            def _():
                row_hop(k).start()

        def row_begin(k):
            y = {}
            for g in range(every):
                y[0, g] = yr[k, g]
                y[1, g] = mul_few(yr[k, g], wc.at[0, g]) + offy[0, g]
            for l, g in each:
                begun[l, g] = y[l, g]
            return y

        def row_coarse():
            for l, g in each:
                begun[l, g] = mul_few(begun[l, g], wc.at[l, g])

        def row_offsets(y):
            for l, g in each:
                offy[l, g] = y[l, g] - begun[l, g]

        def exchange_one(turn, own, work):
            sbuf[turn] = own
            for slot, peer in enumerate(far_peers):
                send(sbuf.at[turn], rbuf.at[turn, slot], ssem.at[turn], rsem.at[turn], peer)
            work()
            arrived(rbuf.at[turn], rsem.at[turn])
            return (own + jnp.sum(rbuf[turn], axis=0)) * (1.0 / cells)

        def exchange_many(turn, own, work):
            part = pl.ds(0, own.shape[0])
            many_s[turn, part] = own
            for slot, peer in enumerate(far_peers):
                send(
                    many_s.at[turn, part], many_r.at[turn, slot, part],
                    mssem.at[turn], mrsem.at[turn], peer,
                )
            work()
            arrived(many_r.at[turn, :, part], mrsem.at[turn])
            return (own + jnp.sum(many_r[turn, :, part], axis=0)) * (1.0 / cells)

        def partial(y, l):
            return total_rows(jnp.where(cell_row, sum(y[l, g][0:8] for g in range(every)), 0.0))

        def advance(y, m, average):
            made = {}
            for l, g in each:
                old = y[l, g]
                size = old.shape[0]
                fed = old * keep + sums[l, g, 0:size]
                if average is not None:
                    fed = fed + weights_n[g] * average[l]
                new = mul_few(fed, wf.at[l, g])
                made[l, g] = jnp.where(limits[0:size] > m, new, old) if m >= FEWEST else new
            return made

        def through(row, l, i):
            return mul_few(jnp.broadcast_to(row, (8, width)), wk.at[l, i])[0:1]

        def late(y, turn, work):
            free = [y]
            for m in (5, 6):
                tops = {k: v[0:8] for k, v in free[-1].items()}
                free.append(advance(tops, m, None))
            own = jnp.concatenate([partial(f, l) for l in range(lead) for f in free], axis=0)
            got = exchange_many(turn, own, work)
            fifth = [got[3 * l : 3 * l + 1] for l in range(lead)]
            y = advance(y, 5, fifth)
            sixth, seventh = [], []
            for l in range(lead):
                free_sixth = got[3 * l + 1 : 3 * l + 2]
                sixth.append(free_sixth + through(fifth[l], l, 0))
                seventh.append(
                    got[3 * l + 2 : 3 * l + 3] + through(fifth[l], l, 2) + through(free_sixth, l, 1)
                )
            y = advance(y, 6, sixth)
            return advance(y, 7, seventh)

        @pl.when(tm == 0)
        def _():
            row_hop(0).start()

        @pl.when(tm > 0)
        def _():
            prepare()
            row_chain(0)
            row_begin(0)

        y = {(l, g): begun[l, g] for l, g in each}

        def beside(m):
            def work():
                if m == 0:
                    @pl.when(tm == 0)
                    def _():
                        prepare()
                        for k in range(ITERS + 1):
                            yr[k] = yinit[...]

                    await_copies(10, 11)
                    for g in range(groups):
                        for l in range(lead):
                            put_weights(wf.at[l, groups + g], fine_p[l, g])
                    x_reduce_start(0)
                    row_coarse()
                elif m == 1:
                    y_reduce_start(0)
                    x_reduce_start(1)
                    bulk_chain(0)
                elif m == 2:
                    y_gather_start(0)
                    bulk_begin(0)
                    for i in range(4):
                        fine_cells(i)
                elif m == 3:
                    x_gather_start(0)
                    y_reduce_start(1)
                    for i in range(4, FINE_MAX):
                        fine_cells(i)
                    bulk_offsets(0)
                elif m == 4:
                    y_gather_start(1)
                    x_gather_done(0)
                    bulk_chain(1)
                else:
                    x_gather_start(1)
                    bulk_begin(1)
                    for i in range(4):
                        fine_cells(i)
                    k_finish(0)

            return work

        for m in range(5):
            own = jnp.concatenate([partial(y, l) for l in range(lead)], axis=0)
            average = exchange_one(m, own, beside(m))
            y = advance(y, m, [average[l : l + 1] for l in range(lead)])
        row_offsets(late(y, 0, beside(5)))
        row_chain(1)

        y = row_begin(1)
        free = [{k: v[0:8] for k, v in y.items()}]
        for m in range(4):
            free.append(advance(free[-1], m, None))
        own = jnp.concatenate([partial(f, l) for l in range(lead) for f in free], axis=0)

        def work():
            row_coarse()
            for m in range(4, FINE_MAX):
                fine_cells(m)
            x_gather_done(1)
            k_finish(1)

        got = exchange_many(1, own, work)
        averages = [[got[5 * l + m : 5 * l + m + 1] for m in range(5)] for l in range(lead)]
        for l in range(lead):
            free_rows = jnp.concatenate(averages[l] + [jnp.zeros((3, width), F32)], axis=0)
            for d in range(1, 5):
                fed = mul_few(free_rows, wl.at[l, d - 1])
                for m in range(d, 5):
                    averages[l][m] = averages[l][m] + fed[m - d : m - d + 1]
        for m in range(5):
            y = advance(y, m, [averages[l][m] for l in range(lead)])

        def work():
            bulk_offsets(1)
            bulk_chain(2)
            bulk_result()

        row_offsets(late(y, 2, work))
        row_chain(2)
        def ends(these):
            for g in these:
                fin[0, g] = mul_few(yr[ITERS, g], wc.at[0, g]) + offy[0, g]
                fin[1, g] = ys[ITERS, g]

        ends(range(groups, every))
        for l in range(lead):
            send(fin.at[l, partner_groups], fin_p.at[l], pssem.at[11 + l], prsem.at[11], partner)
        ends(range(groups))
        result(lambda l, g: fin[l, g])

        for turn in range(5):
            arrived(rbuf.at[turn], ssem.at[turn])
        for turn, size in ((0, 6), (1, 10), (2, 6)):
            arrived(many_r.at[turn, :, pl.ds(0, size)], mssem.at[turn])
        for l in range(lead):
            arrived(fin_p.at[l], pssem.at[11 + l])
        drain_common()

        @pl.when(tm < last)
        def _():
            for k in range(ITERS + 1):
                row_hop(k).wait_send()


def body(initial, source, mix_rate, fine_inverse, coarse_inverse, step_counts):
    lead, count, width = source.shape
    groups = fine_inverse.shape[1]
    every = 2 * groups
    far = XS * YS - 1
    mats = 2 * XS
    vmem = pl.BlockSpec(memory_space=pltpu.VMEM)
    return pl.pallas_call(
        kernel,
        out_shape=jax.ShapeDtypeStruct(source.shape, F32),
        in_specs=[vmem] * 6,
        out_specs=vmem,
        scratch_shapes=[
            pltpu.VMEM((lead, every, 2 * width, 2 * width), BF16),
            pltpu.VMEM((lead, every, 2 * width, 2 * width), BF16),
            pltpu.VMEM((every, 2 * width, 2 * width), BF16),
            pltpu.VMEM((lead, mats, 2 * width, 2 * width), BF16),
            pltpu.VMEM((lead, XS, width, 2 * width), BF16),
            pltpu.VMEM((lead, count, width), F32),
            pltpu.VMEM((lead, count, width), F32),
            pltpu.VMEM((lead, count, width), F32),
            pltpu.VMEM((count, width), F32),
            pltpu.VMEM((groups, count // groups, width), F32),
            pltpu.VMEM((lead, every, 16, width), F32),
            pltpu.VMEM((every, 16, width), F32),
            pltpu.VMEM((every, 16, width), F32),
            pltpu.VMEM((lead, groups, width, width), F32),
            pltpu.VMEM((lead, groups, width, width), F32),
            pltpu.VMEM((lead, every, 16, width), F32),
            pltpu.VMEM((lead, every, 16, width), F32),
            pltpu.VMEM((5, lead, width), F32),
            pltpu.VMEM((5, far, lead, width), F32),
            pltpu.VMEM((3, 16, width), F32),
            pltpu.VMEM((3, far, 16, width), F32),
            pltpu.VMEM((ITERS + 1, count, width), F32),
            pltpu.VMEM((ITERS + 1, count, width), F32),
            pltpu.VMEM((ITERS + 1, every, 16, width), F32),
            pltpu.VMEM((ITERS + 1, every, 16, width), F32),
            pltpu.VMEM((lead, every, 16, width), F32),
            pltpu.VMEM((lead, groups, 16, width), F32),
            pltpu.VMEM((lead, mats, width, width), F32),
            pltpu.VMEM((mats, width, width), F32),
            pltpu.VMEM((mats, width, width), F32),
            pltpu.VMEM((2, XS - 1, width, width), F32),
            pltpu.VMEM((2, width, width), F32),
            pltpu.VMEM((2, YS - 1, width // YS, width), F32),
            pltpu.VMEM((2, width // YS, width), F32),
            pltpu.VMEM((2, width, width), F32),
            pltpu.VMEM((lead, mats, width, width), F32),
            pltpu.SemaphoreType.DMA((5,)),
            pltpu.SemaphoreType.DMA((5,)),
            pltpu.SemaphoreType.DMA((3,)),
            pltpu.SemaphoreType.DMA((3,)),
            pltpu.SemaphoreType.DMA(((ITERS + 1) * NCHUNK,)),
            pltpu.SemaphoreType.DMA(((ITERS + 1) * NCHUNK,)),
            pltpu.SemaphoreType.DMA((ITERS + 1,)),
            pltpu.SemaphoreType.DMA((ITERS + 1,)),
            pltpu.SemaphoreType.DMA((12,)),
            pltpu.SemaphoreType.DMA((12,)),
            pltpu.SemaphoreType.DMA((13,)),
            pltpu.SemaphoreType.DMA((13,)),
        ],
        compiler_params=pltpu.CompilerParams(collective_id=0, has_side_effects=True),
    )(
        initial,
        source,
        mix_rate.reshape(1, width),
        fine_inverse,
        coarse_inverse,
        step_counts.reshape(groups, count // groups),
    )


def solution(mesh):
    return jax.shard_map(
        body,
        mesh=mesh,
        in_specs=(
            P("cell", None),
            P("tm", "cell", None),
            P(),
            P("tm", "cell", None, None),
            P("tm", "cell", None, None),
            P("cell"),
        ),
        out_specs=P("tm", "cell", None),
        check_vma=False,
    )
```
